16 devices in a mesh: dp: 2 (over y, z), tp: 8 (over x, core).
Axes of the slice: x: 4, y: 2, z: 1, core: 2. Of those that a mesh axis runs over, the one named last changes fastest.
The devices are a block of a 4x4x8 slice.
Arguments:
- x: bfloat16 [8, 512, 5120], P('dp'), parts along dimension 0
- gain_a: bfloat16 [5120], replicated
- wq: bfloat16 [5120, 4096], P(None, 'tp')
- wk: bfloat16 [5120, 1024], P(None, 'tp')
- wv: bfloat16 [5120, 1024], P(None, 'tp')
- wo: bfloat16 [4096, 5120], P('tp')
- gain_m: bfloat16 [5120], replicated
- w_gate: bfloat16 [5120, 14336], P(None, 'tp')
- w_up: bfloat16 [5120, 14336], P(None, 'tp')
- w_down: bfloat16 [14336, 5120], P('tp')
Outputs:
- output: bfloat16 [8, 512, 5120], P('dp'), parts along dimension 0
There are 2 independent parts. The reference program is written for one: setup_inputs(seed, part) draws one part's arguments, and reference() takes and returns one part's arrays. A program takes and returns all parts, laid end to end along the dimension named above; an argument that names none is the same for every part.
All inputs are finite; a program needn't handle non-finite values.
Results may differ from the reference program's by a relative error of at most 0.017.
Values are sent between devices in bfloat16 or wider.
A program may use at most 768 MiB of HBM per device.

```python
import jax
import jax.numpy as jnp
from jax import lax

SEQUENCES = 4
TOKENS = 512
D = 5120
HEADS = 32
KV_HEADS = 8
HEAD = 128
FF = 14336
THETA = 10000


def setup_inputs(seed: int = 0, part: int = 0) -> dict:
    kx, ka, km, kq, kk, kv, ko, kg, ku, kd = jax.random.split(jax.random.key(seed), 10)

    def weights(key, rows, columns):
        return jax.random.normal(key, (rows, columns), jnp.float32) * rows**-0.5

    drawn = {
        "x": jax.random.normal(jax.random.fold_in(kx, part), (SEQUENCES, TOKENS, D), jnp.float32),
        "gain_a": 1 + 0.1 * jax.random.normal(ka, (D,), jnp.float32),
        "wq": 2 * weights(kq, D, HEADS * HEAD),
        "wk": 2 * weights(kk, D, KV_HEADS * HEAD),
        "wv": 4 * weights(kv, D, KV_HEADS * HEAD),
        "wo": weights(ko, HEADS * HEAD, D),
        "gain_m": 1 + 0.1 * jax.random.normal(km, (D,), jnp.float32),
        "w_gate": weights(kg, D, FF),
        "w_up": weights(ku, D, FF),
        "w_down": 3 * weights(kd, FF, D),
    }
    return {k: v.astype(jnp.bfloat16) for k, v in drawn.items()}


def normed(x, gain):
    wide = x.astype(jnp.float32)
    scale = lax.rsqrt(jnp.mean(wide * wide, -1, keepdims=True) + 1e-6)
    return (wide * scale * gain.astype(jnp.float32)).astype(jnp.bfloat16)


def turned(t, place, theta):
    half = t.shape[-1] // 2
    angle = place.astype(jnp.float32)[:, None] * theta ** (-jnp.arange(half, dtype=jnp.float32) / half)
    cos, sin = jnp.cos(angle)[:, None], jnp.sin(angle)[:, None]
    a, b = t[..., :half].astype(jnp.float32), t[..., half:].astype(jnp.float32)
    return jnp.concatenate([a * cos - b * sin, b * cos + a * sin], -1).astype(jnp.bfloat16)


def matmul(a, w):
    return jnp.dot(a, w, preferred_element_type=jnp.float32).astype(jnp.bfloat16)


def einsum(form, a, b):
    return jnp.einsum(form, a.astype(jnp.float32), b.astype(jnp.float32))


def attention(q, k, v):
    scores = einsum("tgsd,ugd->gstu", q, k) * q.shape[-1] ** -0.5
    token = jnp.arange(q.shape[0])
    scores = jnp.where(token[:, None] >= token, scores, -jnp.inf)
    weights = jax.nn.softmax(scores, -1).astype(jnp.bfloat16)
    return einsum("gstu,ugd->tgsd", weights, v).astype(jnp.bfloat16)


def one(x, gain_a, wq, wk, wv, wo, gain_m, w_gate, w_up, w_down):
    rows = x.shape[0]
    a, place = normed(x, gain_a), jnp.arange(rows)
    k = turned(matmul(a, wk).reshape(rows, -1, HEAD), place, THETA)
    q = turned(matmul(a, wq).reshape(rows, -1, HEAD), place, THETA).reshape(rows, k.shape[1], -1, HEAD)
    v = matmul(a, wv).reshape(rows, -1, HEAD)
    seen = attention(q, k, v).reshape(rows, -1)
    h = (x.astype(jnp.float32) + jnp.dot(seen, wo, preferred_element_type=jnp.float32)).astype(jnp.bfloat16)
    b = normed(h, gain_m)
    gate = jnp.dot(b, w_gate, preferred_element_type=jnp.float32)
    up = jnp.dot(b, w_up, preferred_element_type=jnp.float32)
    hidden = (jax.nn.silu(gate) * up).astype(jnp.bfloat16)
    return (h.astype(jnp.float32) + jnp.dot(hidden, w_down, preferred_element_type=jnp.float32)).astype(jnp.bfloat16)


def reference(x, gain_a, wq, wk, wv, wo, gain_m, w_gate, w_up, w_down):
    return lax.map(lambda sequence: one(sequence, gain_a, wq, wk, wv, wo, gain_m, w_gate, w_up, w_down), x)
```

```python
import functools

import jax
import jax.numpy as jnp
from jax import lax
from jax.experimental import pallas as pl
from jax.experimental.pallas import tpu as pltpu
from jax.sharding import PartitionSpec as P

HEAD = 128
THETA = 10000
MESH = pl.DeviceIdType.MESH
HIDDEN = -1e30
LOG2E = 1.4426950408889634
CORES = 2
SUBS = 2
SLOTS = 12
LAG = 3
WIDE = 512
EPS = 1e-6


def _kernel(x_ref, ga, gm, cs, sn, wq, wk, wv, wo, wg, wu, wd, buf, act, own, land, stage, arr, sbuf, res, bsh, w1, w2, qs, ks, vs, seen,
            hid, r256, r512, act_sem, res_sem, w1_sem, w2_sem, st_send, d2d_recv, rs_send, rs_recv, ag_send, ag_recv, ag_dsend, ag_drecv,
            ag_loc, credit, *, tp):
    chunks, rows, d = x_ref.shape
    chips = tp // CORES
    half_rows = rows // CORES
    share = half_rows // chips
    piece = share // (2 * SUBS)
    tiles = d // WIDE
    heads = wq.shape[1] // HEAD
    ff = wg.shape[1]
    up_tiles = ff // HEAD
    q_tiles = wq.shape[1] // 256
    a_tiles = q_tiles + 1
    units = 4 * chunks // 2
    steps = (chips - 1) * SUBS
    me = lax.axis_index("tp")
    chip, core = lax.div(me, CORES), lax.rem(me, CORES)
    partner = me + 1 - 2 * core
    right, left = lax.rem(me + CORES, tp), lax.rem(me + tp - CORES, tp)
    mine = pl.multiple_of(core * half_rows, half_rows)
    theirs = pl.multiple_of((1 - core) * half_rows, half_rows)

    def to(device):
        return dict(device_id={"tp": device}, device_id_type=MESH)

    def side(way):
        return jnp.where(way == 0, right, left)

    def place(way, hops):
        return lax.rem(chip + 2 * chips + jnp.where(way == 0, -hops, hops), chips)

    barrier = pltpu.get_barrier_semaphore()
    for other in (left, right, partner):
        pl.semaphore_signal(barrier, inc=1, **to(other))
    pl.semaphore_wait(barrier, 3)

    def act_copy(m):
        return pltpu.make_async_copy(buf.at[lax.rem(m, chunks)], act, act_sem)

    def load_act(m):
        @pl.when(m < chunks)
        def _():
            pltpu.make_async_copy(x_ref.at[lax.rem(m, chunks)], act, act_sem).start()

        @pl.when(m >= chunks)
        def _():
            act_copy(m).start()

    a_total = a_tiles * chunks

    def load_w1(n):
        par = lax.rem(n, 2)
        ja = lax.rem(n, a_tiles)

        @pl.when((n < a_total) & (ja < q_tiles))
        def _():
            pltpu.make_async_copy(wq.at[:, pl.ds(pl.multiple_of(ja * 256, 256), 256)], w1.at[par], w1_sem.at[par]).start()

        def pair(a, b, at):
            pltpu.make_async_copy(a.at[:, pl.ds(at, HEAD)], w1.at[par, :, pl.ds(0, HEAD)], w1_sem.at[par]).start()
            pltpu.make_async_copy(b.at[:, pl.ds(at, HEAD)], w1.at[par, :, pl.ds(HEAD, HEAD)], w1_sem.at[par]).start()

        @pl.when((n < a_total) & (ja == q_tiles))
        def _():
            pair(wk, wv, 0)

        @pl.when((n >= a_total) & (n < a_total + up_tiles * chunks))
        def _():
            pair(wg, wu, pl.multiple_of(lax.rem(n - a_total, up_tiles) * HEAD, HEAD))

    def w2_copy(first, j):
        par = lax.rem(j, 2)
        at = pl.ds(pl.multiple_of(j * WIDE, WIDE), WIDE)
        if first:
            return pltpu.make_async_copy(wo.at[:, at], w2.at[par, pl.ds(0, wo.shape[0])], w2_sem.at[par])
        return pltpu.make_async_copy(wd.at[:, at], w2.at[par], w2_sem.at[par])

    def load_w2(m, j):
        @pl.when(m < chunks)
        def _():
            w2_copy(True, j).start()

        @pl.when(m >= chunks)
        def _():
            w2_copy(False, j).start()

    def norm_act():
        def block(r, _):
            at = pl.ds(pl.multiple_of(r * 16, 16), 16)
            wide = act[at, :].astype(jnp.float32)
            scale = lax.rsqrt(jnp.mean(wide * wide, -1, keepdims=True) + EPS)
            act[at, :] = (wide * scale * ga[...].astype(jnp.float32)).astype(jnp.bfloat16)
            return 0

        lax.fori_loop(0, rows // 16, block, 0)

    def turned(t):
        wide = t.astype(jnp.bfloat16).astype(jnp.float32)
        return (wide * cs[...] + pltpu.roll(wide, HEAD // 2, 1) * sn[...]).astype(jnp.bfloat16)

    def attention(head):
        e = HEAD**-0.5 * LOG2E
        for r in range(2):
            n, keys = rows // 2, (r + 1) * rows // 2
            q = qs[head, r * n : (r + 1) * n, :]
            s = lax.dot_general(q, ks[:keys, :], (((1,), (1,)), ((), ())), preferred_element_type=jnp.float32)
            gap = lax.broadcasted_iota(jnp.int32, s.shape, 0) + r * n - lax.broadcasted_iota(jnp.int32, s.shape, 1)
            s = jnp.where(gap >= 0, s, HIDDEN)
            p = jnp.exp2((s - s.max(-1, keepdims=True)) * e)
            o = jnp.dot(p.astype(jnp.bfloat16), vs[:keys, :], preferred_element_type=jnp.float32)
            o = o * (1 / p.sum(-1, keepdims=True))
            seen[r * n : (r + 1) * n, pl.ds(pl.multiple_of(head * HEAD, HEAD), HEAD)] = o.astype(jnp.bfloat16)

    def compute(g, _):
        m, i = lax.div(g, SLOTS), lax.rem(g, SLOTS)
        first = m < chunks
        slot = lax.rem(m, 3)

        @pl.when(i == 0)
        def _():
            act_copy(0).wait()

        @pl.when((i == 0) & first)
        def _():
            norm_act()

        def tile1(jj, _):
            n = jnp.where(first, a_tiles * m + i, a_total + up_tiles * (m - chunks) + 2 * i + jj)
            par = lax.rem(n, 2)
            pltpu.make_async_copy(w1.at[par], w1.at[par], w1_sem.at[par]).wait()
            load_w1(n + 1)
            r256[...] = jnp.dot(act[...], w1[par], preferred_element_type=jnp.float32)

            @pl.when(first & (i < q_tiles))
            def _():
                qs[2 * i] = turned(r256[:, :HEAD])
                qs[2 * i + 1] = turned(r256[:, HEAD:])

            @pl.when(first & (i == q_tiles))
            def _():
                ks[...] = turned(r256[:, :HEAD])
                vs[...] = r256[:, HEAD:].astype(jnp.bfloat16)

            @pl.when(jnp.logical_not(first))
            def _():
                at = pl.ds(pl.multiple_of((2 * i + jj) * HEAD, HEAD), HEAD)
                hid[:, at] = (jax.nn.silu(r256[:, :HEAD]) * r256[:, HEAD:]).astype(jnp.bfloat16)

            return 0

        count1 = jnp.where(first, jnp.where(i < a_tiles, 1, 0), jnp.where(i < up_tiles // 2, 2, 0))
        lax.fori_loop(0, count1, tile1, 0)

        @pl.when(first & (i >= a_tiles) & (i < a_tiles + heads))
        def _():
            attention(i - a_tiles)

        @pl.when(i == 3)
        def _():
            load_w2(m, 0)

        last = SLOTS - tiles // 2

        @pl.when((i == last) & (m < 2 * chunks - 1))
        def _():
            load_act(m + 1)

        @pl.when((i == last) & (m >= 3))
        def _():
            pl.semaphore_wait(credit.at[slot], 1)

        def tile2(jj, _):
            j = 2 * (i - last) + jj
            par = lax.rem(j, 2)

            @pl.when(first)
            def _():
                w2_copy(True, j).wait()

            @pl.when(jnp.logical_not(first))
            def _():
                w2_copy(False, j).wait()

            @pl.when(j + 1 < tiles)
            def _():
                load_w2(m, j + 1)

            @pl.when(first)
            def _():
                r512[...] = jnp.dot(seen[...], w2[par, : wo.shape[0], :], preferred_element_type=jnp.float32)

            @pl.when(jnp.logical_not(first))
            def _():
                r512[...] = jnp.dot(hid[...], w2[par], preferred_element_type=jnp.float32)

            copy = pltpu.make_async_remote_copy(stage.at[par], land.at[slot, j], st_send.at[par], d2d_recv.at[slot], **to(partner))

            @pl.when(m * tiles + j >= 2)
            def _():
                copy.wait_send()

            stage[par] = r512[pl.ds(theirs, half_rows), :].astype(jnp.bfloat16)
            copy.start()
            own[slot, j] = r512[pl.ds(mine, half_rows), :]
            return 0

        lax.fori_loop(0, jnp.where(i >= last, 2, 0), tile2, 0)
        return 0

    def at_arr(lane, way, s, sub):
        return ((lane * 2 + way) * (chips - 1) + s) * SUBS + sub

    def at_sbuf(lane, way, s, sub):
        return ((lane * 2 + way) * 2 + lax.rem(s, 2)) * SUBS + sub

    def row_of(there, way, sub):
        return pl.multiple_of(there * share + way * (share // 2) + sub * piece, piece)

    def rs_copy(lane, way, s, sub):
        return pltpu.make_async_remote_copy(
            sbuf.at[at_sbuf(lane, way, s, sub)], arr.at[at_arr(lane, way, s, sub)], rs_send.at[at_sbuf(lane, way, s, sub)],
            rs_recv.at[at_arr(lane, way, s, sub)], **to(side(way)))

    def cols(t):
        return pl.ds(pl.multiple_of(t * WIDE, WIDE), WIDE)

    def local(slot, row, t):
        at = pl.ds(row, piece)
        return own[slot, t, at, :] + land[slot, t, at, :].astype(jnp.float32)

    def rs_start(lane, slot):
        pltpu.make_async_copy(land.at[slot], land.at[slot], d2d_recv.at[slot]).wait()

        def one(z, _):
            sub, way = lax.div(z, 2), lax.rem(z, 2)
            row, out = row_of(place(way, 1), way, sub), at_sbuf(lane, way, 0, sub)

            def add(t, _):
                sbuf[out, :, cols(t)] = local(slot, row, t).astype(jnp.bfloat16)
                return 0

            lax.fori_loop(0, tiles, add, 0)
            rs_copy(lane, way, 0, sub).start()
            return 0

        lax.fori_loop(0, 2 * SUBS, one, 0)

    def rs_step(lane, slot, s, sub):
        def one(way, _):
            row, out, into = row_of(place(way, s + 2), way, sub), at_sbuf(lane, way, s + 1, sub), at_arr(lane, way, s, sub)
            rs_copy(lane, way, s, sub).wait_recv()

            def add(t, _):
                sbuf[out, :, cols(t)] = (local(slot, row, t) + arr[into, :, cols(t)].astype(jnp.float32)).astype(jnp.bfloat16)
                return 0

            lax.fori_loop(0, tiles, add, 0)
            rs_copy(lane, way, s + 1, sub).start()
            rs_copy(lane, way, s, sub).wait_send()
            return 0

        lax.fori_loop(0, 2, one, 0)

    def rs_last(lane, slot, chunk, half, sub):
        s = chips - 2

        def one(way, _):
            row, into = row_of(chip, way, sub), at_arr(lane, way, s, sub)
            rs_copy(lane, way, s, sub).wait_recv()
            at = pl.ds(row_of(0, way, sub), piece)

            def add(t, square):
                total = local(slot, row, t) + arr[into, :, cols(t)].astype(jnp.float32)
                new = (res[chunk, at, cols(t)].astype(jnp.float32) + total).astype(jnp.bfloat16)
                res[chunk, at, cols(t)] = new
                wide = new.astype(jnp.float32)
                return square + wide * wide

            square = lax.fori_loop(0, tiles, add, jnp.zeros((piece, WIDE), jnp.float32))
            scale = lax.rsqrt(jnp.sum(square, -1, keepdims=True) / d + EPS)

            @pl.when(half == 0)
            def _():
                def put(t, _):
                    wide = res[chunk, at, cols(t)].astype(jnp.float32)
                    bsh[lane, at, cols(t)] = (wide * scale * gm[:, cols(t)].astype(jnp.float32)).astype(jnp.bfloat16)
                    return 0

                lax.fori_loop(0, tiles, put, 0)

            @pl.when(half == 1)
            def _():
                def put(t, _):
                    bsh[lane, at, cols(t)] = res[chunk, at, cols(t)]
                    return 0

                lax.fori_loop(0, tiles, put, 0)

            rs_copy(lane, way, s, sub).wait_send()
            return 0

        lax.fori_loop(0, 2, one, 0)

    def ag_copy(source, lane, which, there, way, s, sub):
        at = buf.at[which, pl.ds(mine + row_of(there, way, sub), piece)]
        return pltpu.make_async_remote_copy(at if source is None else source, at, ag_send.at[lane], ag_recv.at[at_arr(lane, way, s, sub)],
                                            **to(side(way)))

    def ag_over(source, lane, which, row, count):
        at = buf.at[which, pl.ds(mine + row, count)]
        return pltpu.make_async_remote_copy(at if source is None else source, at, ag_dsend.at[lane], ag_drecv.at[which], **to(partner))

    def ag_start(lane, which):
        def one(z, _):
            sub, way = lax.div(z, 2), lax.rem(z, 2)
            ag_copy(bsh.at[lane, pl.ds(row_of(0, way, sub), piece)], lane, which, chip, way, 0, sub).start()
            return 0

        lax.fori_loop(0, 2 * SUBS, one, 0)
        ag_over(bsh.at[lane], lane, which, row_of(chip, 0, 0), share).start()
        pltpu.make_async_copy(bsh.at[lane], buf.at[which, pl.ds(mine + row_of(chip, 0, 0), share)], ag_loc.at[lane]).start()

    def ag_step(lane, which, s, sub):
        def one(way, _):
            there = place(way, s + 1)
            ag_copy(None, lane, which, there, way, s, sub).wait_recv()

            @pl.when(s < chips - 2)
            def _():
                ag_copy(None, lane, which, there, way, s + 1, sub).start()

            ag_over(None, lane, which, row_of(there, way, sub), piece).start()
            return 0

        lax.fori_loop(0, 2, one, 0)

    def ag_end(lane, which):
        sent = buf.at[which, pl.ds(0, (chips - 1) * share)]
        pltpu.make_async_copy(sent, sent, ag_send.at[lane]).wait()
        over = buf.at[which, pl.ds(mine, half_rows)]
        pltpu.make_async_copy(over, over, ag_dsend.at[lane]).wait()
        came = buf.at[which, pl.ds(theirs, half_rows)]
        pltpu.make_async_copy(came, came, ag_drecv.at[which]).wait()
        here = buf.at[which, pl.ds(mine + row_of(chip, 0, 0), share)]
        pltpu.make_async_copy(bsh.at[lane], here, ag_loc.at[lane]).wait()

    def unit(lane, k):
        half, phase = lax.div(k, units // 2), lax.rem(k, 2)
        chunk = lane + 2 * lax.rem(lax.div(k, 2), chunks // 2)
        m = chunks * half + chunk
        return half, phase, chunk, m, lax.rem(m, 3)

    def lane_step(q):
        lane = lax.rem(q, 2)
        u = lax.div(q, 2) - LAG * lane

        @pl.when((u >= 1) & (u <= units * steps))
        def _():
            k, e = lax.div(u - 1, steps), lax.rem(u - 1, steps)
            half, phase, chunk, m, slot = unit(lane, k)
            s, sub = lax.div(e, SUBS), lax.rem(e, SUBS)

            @pl.when((phase == 0) & (s < chips - 2))
            def _():
                rs_step(lane, slot, s, sub)

            @pl.when((phase == 0) & (s == chips - 2))
            def _():
                rs_last(lane, slot, chunk, half, sub)

            @pl.when((phase == 0) & (e == steps - 1) & (m + 3 < 2 * chunks))
            def _():
                pl.semaphore_signal(credit.at[slot], inc=1, **to(partner))

            @pl.when(phase == 1)
            def _():
                ag_step(lane, m, s, sub)

            @pl.when((phase == 1) & (e == steps - 1))
            def _():
                ag_end(lane, m)

        @pl.when((u >= 0) & (u < units * steps) & (lax.rem(u, steps) == 0))
        def _():
            half, phase, chunk, m, slot = unit(lane, lax.div(u, steps))

            @pl.when(phase == 0)
            def _():
                rs_start(lane, slot)

            @pl.when(phase == 1)
            def _():
                ag_start(lane, m)

    total = SLOTS * 2 * chunks
    lead = 2 * LAG + 1

    def slots(q):
        early = jnp.where(q <= 0, 0, SLOTS + 2 * (q - 1))
        return jnp.where(q < lead, early, jnp.minimum(2 * SLOTS + q - lead, total))

    load_act(0)
    load_w1(0)
    for n in range(chunks):
        pltpu.make_async_copy(x_ref.at[n, pl.ds(mine + row_of(chip, 0, 0), share)], res.at[n], res_sem).start()

    def body(q, _):
        lax.fori_loop(slots(q), slots(q + 1), compute, 0)

        @pl.when(q == 0)
        def _():
            pltpu.make_async_copy(res, res, res_sem).wait()

        lane_step(q)
        return 0

    lax.fori_loop(0, 2 * (units * steps + LAG + 1), body, 0)
    for par in range(2):
        pltpu.make_async_remote_copy(stage.at[par], land.at[0, 0], st_send.at[par], d2d_recv.at[0], **to(partner)).wait_send()


def solution(mesh):
    tp = mesh.shape["tp"]

    def step(x, gain_a, wq, wk, wv, wo, gain_m, w_gate, w_up, w_down):
        chunks, rows, d = x.shape
        chips = tp // CORES
        half_rows = rows // CORES
        share = half_rows // chips
        piece = share // (2 * SUBS)
        half = HEAD // 2
        angle = jnp.arange(rows).astype(jnp.float32)[:, None] * THETA ** (-jnp.arange(half, dtype=jnp.float32) / half)
        cos, sin = jnp.cos(angle), jnp.sin(angle)
        cs, sn = jnp.concatenate([cos, cos], -1), jnp.concatenate([-sin, sin], -1)
        bf, f32 = jnp.bfloat16, jnp.float32
        vmem, dma = pltpu.VMEM, pltpu.SemaphoreType.DMA
        hbm, inside = pl.BlockSpec(memory_space=pl.ANY), pl.BlockSpec(memory_space=pltpu.VMEM)
        heads, ff = wq.shape[1] // HEAD, w_gate.shape[1]
        n_arr, n_sbuf = 2 * 2 * (chips - 1) * SUBS, 2 * 2 * 2 * SUBS
        buf = pl.pallas_call(
            functools.partial(_kernel, tp=tp),
            out_shape=jax.ShapeDtypeStruct((2 * chunks, rows, d), bf),
            in_specs=[hbm, inside, inside, inside, inside] + [hbm] * 7,
            out_specs=hbm,
            scratch_shapes=[
                vmem((rows, d), bf),
                vmem((3, d // WIDE, half_rows, WIDE), f32),
                vmem((3, d // WIDE, half_rows, WIDE), bf),
                vmem((2, half_rows, WIDE), bf),
                vmem((n_arr, piece, d), bf),
                vmem((n_sbuf, piece, d), bf),
                vmem((chunks, share, d), bf),
                vmem((2, share, d), bf),
                vmem((2, d, 256), bf),
                vmem((2, ff, WIDE), bf),
                vmem((heads, rows, HEAD), bf),
                vmem((rows, HEAD), bf),
                vmem((rows, HEAD), bf),
                vmem((rows, heads * HEAD), bf),
                vmem((rows, ff), bf),
                vmem((rows, 256), f32),
                vmem((rows, WIDE), f32),
                dma, dma, dma((2,)), dma((2,)), dma((2,)), dma((3,)), dma((n_sbuf,)), dma((n_arr,)), dma((2,)), dma((n_arr,)),
                dma((2,)), dma((2 * chunks,)), dma((2,)), pltpu.SemaphoreType.REGULAR((3,)),
            ],
            compiler_params=pltpu.CompilerParams(collective_id=0, has_side_effects=True, vmem_limit_bytes=66 * 10**6),
            name="layer",
        )(x, gain_a.reshape(1, d), gain_m.reshape(1, d), cs, sn, wq, wk, wv, wo, w_gate, w_up, w_down)
        return lax.slice_in_dim(buf, chunks, 2 * chunks, axis=0)

    tokens, whole, columns, rows_of = P("dp", None, None), P(None), P(None, "tp"), P("tp", None)
    return jax.shard_map(
        step,
        mesh=mesh,
        in_specs=(tokens, whole, columns, columns, columns, rows_of, whole, columns, columns, rows_of),
        out_specs=tokens,
        check_vma=False,
    )
```

```python
import functools

import jax
import jax.numpy as jnp
from jax import lax
from jax.experimental import pallas as pl
from jax.experimental.pallas import tpu as pltpu
from jax.sharding import PartitionSpec as P

HEAD = 128
THETA = 10000
MESH = pl.DeviceIdType.MESH
HIDDEN = -1e30
LOG2E = 1.4426950408889634
CORES = 2
SUBS = 2
ATTN = (1, 8), (13, 16), (19, 8)
MLPS = (31, 16), (43, 16), (55, 16), (67, 14)
LAG = 6
DEEP = 3
STAGES = 5
M_PARTS = 2
PARTS = 4
NORM_ROWS = 64
NORM_SLOTS = 2
PAIR = 2
AHEAD = 3
WIDE = 512
EPS = 1e-6


def _kernel(x_ref, ga, gm, cs, sn, wq, wk, wv, wo, wg, wu, wd, buf, act, own, land, stage, arr, sbuf, res, bsh, w1, w2, qs, ks, vs, seen,
            hid, r256, act_sem, res_sem, w1_sem, w2_sem, st_send, d2d_recv, rs_send, rs_recv, ag_send, ag_recv, ag_dsend, ag_drecv,
            ag_loc, credit, *, tp):
    chunks, rows, d = x_ref.shape
    chips = tp // CORES
    half_rows = rows // CORES
    share = half_rows // chips
    piece = share // (2 * SUBS)
    tiles = d // WIDE
    heads = wq.shape[1] // HEAD
    ff = wg.shape[1]
    up_tiles = ff // HEAD
    q_tiles = wq.shape[1] // 256
    a_tiles = q_tiles + 1
    units = 4 * chunks // 2
    steps = (chips - 1) * SUBS
    me = lax.axis_index("tp")
    chip, core = lax.div(me, CORES), lax.rem(me, CORES)
    partner = me + 1 - 2 * core
    right, left = lax.rem(me + CORES, tp), lax.rem(me + tp - CORES, tp)
    mine = pl.multiple_of(core * half_rows, half_rows)
    theirs = pl.multiple_of((1 - core) * half_rows, half_rows)

    def to(device):
        return dict(device_id={"tp": device}, device_id_type=MESH)

    def side(way):
        return jnp.where(way == 0, right, left)

    def place(way, hops):
        return lax.rem(chip + 2 * chips + jnp.where(way == 0, -hops, hops), chips)

    barrier = pltpu.get_barrier_semaphore()
    for other in (left, right, partner):
        pl.semaphore_signal(barrier, inc=1, **to(other))
    pl.semaphore_wait(barrier, 3)

    part = rows // PARTS

    def act_copy(source, m, n):
        at = pl.ds(n * part, part)
        return pltpu.make_async_copy(source.at[lax.rem(m, chunks), at], act.at[at], act_sem.at[n])

    def load_act(m):
        @pl.when(m < chunks)
        def _():
            for n in range(PARTS):
                act_copy(x_ref, m, n).start()

        @pl.when(m >= chunks)
        def _():
            for n in range(PARTS):
                act_copy(buf, m, n).start()

    a_total = a_tiles * chunks

    def load_w1(n):
        par = lax.rem(n, DEEP)
        ja = lax.rem(n, a_tiles)

        @pl.when((n < a_total) & (ja < q_tiles))
        def _():
            pltpu.make_async_copy(wq.at[:, pl.ds(pl.multiple_of(ja * 256, 256), 256)], w1.at[par], w1_sem.at[par]).start()

        def pair(a, b, at):
            pltpu.make_async_copy(a.at[:, pl.ds(at, HEAD)], w1.at[par, :, pl.ds(0, HEAD)], w1_sem.at[par]).start()
            pltpu.make_async_copy(b.at[:, pl.ds(at, HEAD)], w1.at[par, :, pl.ds(HEAD, HEAD)], w1_sem.at[par]).start()

        @pl.when((n < a_total) & (ja == q_tiles))
        def _():
            pair(wk, wv, 0)

        @pl.when((n >= a_total) & (n < a_total + up_tiles * chunks))
        def _():
            pair(wg, wu, pl.multiple_of(lax.rem(n - a_total, up_tiles) * HEAD, HEAD))

    deep_rows = wo.shape[0]
    pack = ff // deep_rows
    groups = -(-tiles // pack)

    def w2_slot(m, j):
        first = m < chunks
        return lax.rem(jnp.where(first, groups * m + lax.div(j, pack), groups * chunks + tiles * (m - chunks) + j), DEEP)

    def wo_copy(m, j):
        at = pl.ds(pl.multiple_of(lax.rem(j, pack) * deep_rows, deep_rows), deep_rows)
        par = w2_slot(m, j)
        return pltpu.make_async_copy(wo.at[:, pl.ds(pl.multiple_of(j * WIDE, WIDE), WIDE)], w2.at[par, at], w2_sem.at[par])

    def wd_copy(m, j):
        par = w2_slot(m, j)
        return pltpu.make_async_copy(wd.at[:, pl.ds(pl.multiple_of(j * WIDE, WIDE), WIDE)], w2.at[par], w2_sem.at[par])

    def load_wo(m, group):
        def one(z, _):
            wo_copy(m, group * pack + z).start()
            return 0

        lax.fori_loop(0, jnp.minimum(pack, tiles - group * pack), one, 0)

    def norm_act(first_part):
        for n in range(first_part, first_part + PARTS // NORM_SLOTS):
            act_copy(x_ref, 0, n).wait()

            def block(r, _):
                scales, ats = [], [pl.ds(pl.multiple_of(n * part + r * NORM_ROWS + z * 16, 16), 16) for z in range(NORM_ROWS // 16)]
                for at in ats:
                    square = jnp.zeros((16, WIDE), jnp.float32)
                    for t in range(tiles):
                        wide = act[at, t * WIDE : (t + 1) * WIDE].astype(jnp.float32)
                        square += wide * wide
                    scales.append(lax.rsqrt(jnp.sum(square, -1, keepdims=True) / d + EPS))
                for at, scale in zip(ats, scales):
                    for t in range(tiles):
                        wide = act[at, t * WIDE : (t + 1) * WIDE].astype(jnp.float32)
                        act[at, t * WIDE : (t + 1) * WIDE] = (wide * scale * ga[:, t * WIDE : (t + 1) * WIDE]).astype(jnp.bfloat16)
                return 0

            lax.fori_loop(0, part // NORM_ROWS, block, 0)

    def turned(t):
        wide = t.astype(jnp.bfloat16).astype(jnp.float32)
        return (wide * cs[...] + pltpu.roll(wide, HEAD // 2, 1) * sn[...]).astype(jnp.bfloat16)

    def attention(i):
        e = HEAD**-0.5 * LOG2E
        for r in range(2):
            for z in range(PAIR):
                head = PAIR * i + z
                n, keys = rows // 2, (r + 1) * rows // 2
                q = qs[head, r * n : (r + 1) * n, :]
                s = lax.dot_general(q, ks[:keys, :], (((1,), (1,)), ((), ())), preferred_element_type=jnp.float32)
                gap = lax.broadcasted_iota(jnp.int32, s.shape, 0) + r * n - lax.broadcasted_iota(jnp.int32, s.shape, 1)
                s = jnp.where(gap >= 0, s, HIDDEN)
                p = jnp.exp2((s - s.max(-1, keepdims=True)) * e)
                o = jnp.dot(p.astype(jnp.bfloat16), vs[:keys, :], preferred_element_type=jnp.float32)
                o = o * (1 / p.sum(-1, keepdims=True))
                seen[r * n : (r + 1) * n, pl.ds(pl.multiple_of(head * HEAD, HEAD), HEAD)] = o.astype(jnp.bfloat16)

    b_slots = NORM_SLOTS + a_tiles
    a_slots, m_slots = b_slots + heads // PAIR + tiles // 2, up_tiles + tiles

    def compute(g, _):
        first = g < a_slots * chunks
        after = g - a_slots * chunks
        m = jnp.where(first, lax.div(g, a_slots), chunks + lax.div(after, m_slots))
        i = jnp.where(first, lax.rem(g, a_slots), lax.rem(after, m_slots))
        slot = lax.rem(m, 3)

        for n in range(NORM_SLOTS):

            @pl.when((i == n) & first)
            def _():
                norm_act(n * (PARTS // NORM_SLOTS))

        @pl.when((i == 0) & jnp.logical_not(first))
        def _():
            for n in range(PARTS):
                act_copy(buf, 0, n).wait()

        def tile1(n):
            par = lax.rem(n, DEEP)
            pltpu.make_async_copy(w1.at[par], w1.at[par], w1_sem.at[par]).wait()
            load_w1(n + DEEP - 1)
            return par

        @pl.when(first & (i >= NORM_SLOTS) & (i < b_slots))
        def _():
            j = i - NORM_SLOTS
            par = tile1(a_tiles * m + j)
            r256[...] = jnp.dot(act[...], w1[par], preferred_element_type=jnp.float32)

            @pl.when(j < q_tiles)
            def _():
                qs[2 * j] = turned(r256[:, :HEAD])
                qs[2 * j + 1] = turned(r256[:, HEAD:])

            @pl.when(j == q_tiles)
            def _():
                ks[...] = turned(r256[:, :HEAD])
                vs[...] = r256[:, HEAD:].astype(jnp.bfloat16)

        @pl.when(jnp.logical_not(first) & (i < up_tiles))
        def _():
            par = tile1(a_total + up_tiles * (m - chunks) + i)
            at = pl.ds(pl.multiple_of(i * HEAD, HEAD), HEAD)
            for r in range(0, rows, rows // M_PARTS):
                both = jnp.dot(act[r : r + rows // M_PARTS, :], w1[par], preferred_element_type=jnp.float32)
                hid[r : r + rows // M_PARTS, at] = (jax.nn.silu(both[:, :HEAD]) * both[:, HEAD:]).astype(jnp.bfloat16)

        @pl.when(first & (i >= b_slots) & (i < b_slots + heads // PAIR))
        def _():
            attention(i - b_slots)

        @pl.when(i == 3)
        def _():
            @pl.when(first)
            def _():
                for n in range(DEEP):
                    load_wo(m, n)

            @pl.when(jnp.logical_not(first))
            def _():
                for j in range(DEEP - 1):
                    wd_copy(m, j).start()

        last = jnp.where(first, b_slots + heads // PAIR, up_tiles)

        ahead = jnp.where(m < chunks - 1, last, jnp.where(m == chunks - 1, a_slots - 1, m_slots - 2))

        @pl.when((i == ahead) & (m < 2 * chunks - 1))
        def _():
            load_act(m + 1)

        @pl.when((i == last) & (m >= 3))
        def _():
            pl.semaphore_wait(credit.at[slot], 1)

        def put(j, source, weights):
            out = lax.rem(j, STAGES)
            copy = pltpu.make_async_remote_copy(stage.at[out], land.at[slot, j], st_send.at[out], d2d_recv.at[slot], **to(partner))

            @pl.when(m * tiles + j >= STAGES)
            def _():
                copy.wait_send()

            stage[out] = jnp.dot(source[pl.ds(theirs, half_rows), :], weights, preferred_element_type=jnp.float32).astype(jnp.bfloat16)
            copy.start()
            own[slot, j] = jnp.dot(source[pl.ds(mine, half_rows), :], weights, preferred_element_type=jnp.float32)

        @pl.when(first & (i >= last))
        def _():
            def tile2(jj, _):
                j = 2 * (i - last) + jj
                par = w2_slot(m, j)

                @pl.when(lax.rem(j, pack) == 0)
                def _():
                    def one(z, _):
                        wo_copy(m, j).wait()
                        return 0

                    lax.fori_loop(0, jnp.minimum(pack, tiles - j), one, 0)

                put(j, seen, w2[par, pl.ds(pl.multiple_of(lax.rem(j, pack) * deep_rows, deep_rows), deep_rows), :])

                @pl.when(j == pack - 1)
                def _():
                    for n in range(DEEP, groups):
                        load_wo(m, n)

                return 0

            lax.fori_loop(0, 2, tile2, 0)

        @pl.when(jnp.logical_not(first) & (i >= last))
        def _():
            j = i - last
            wd_copy(m, j).wait()

            @pl.when(j + DEEP - 1 < tiles)
            def _():
                wd_copy(m, j + DEEP - 1).start()

            put(j, hid, w2[w2_slot(m, j)])

        return 0

    def at_arr(lane, way, s, sub):
        return ((lane * 2 + way) * (chips - 1) + s) * SUBS + sub

    def at_sbuf(lane, way, s, sub):
        return ((lane * 2 + way) * 2 + lax.rem(s, 2)) * SUBS + sub

    def row_of(there, way, sub):
        return pl.multiple_of(there * share + way * (share // 2) + sub * piece, piece)

    def rs_copy(lane, way, s, sub):
        return pltpu.make_async_remote_copy(
            sbuf.at[at_sbuf(lane, way, s, sub)], arr.at[at_arr(lane, way, s, sub)], rs_send.at[at_sbuf(lane, way, s, sub)],
            rs_recv.at[at_arr(lane, way, s, sub)], **to(side(way)))

    def cols(t):
        return pl.ds(pl.multiple_of(t * WIDE, WIDE), WIDE)

    def local(slot, row, t):
        at = pl.ds(row, piece)
        return own[slot, t, at, :] + land[slot, t, at, :].astype(jnp.float32)

    def rs_start(lane, slot):
        pltpu.make_async_copy(land.at[slot], land.at[slot], d2d_recv.at[slot]).wait()

        def one(z, _):
            sub, way = lax.div(z, 2), lax.rem(z, 2)
            row, out = row_of(place(way, 1), way, sub), at_sbuf(lane, way, 0, sub)

            def add(t, _):
                sbuf[out, :, cols(t)] = local(slot, row, t).astype(jnp.bfloat16)
                return 0

            lax.fori_loop(0, tiles, add, 0, unroll=True)
            rs_copy(lane, way, 0, sub).start()
            return 0

        lax.fori_loop(0, 2 * SUBS, one, 0)

    def rs_step(lane, slot, s, sub):
        def one(way, _):
            row, out, into = row_of(place(way, s + 2), way, sub), at_sbuf(lane, way, s + 1, sub), at_arr(lane, way, s, sub)
            rs_copy(lane, way, s, sub).wait_recv()

            @pl.when(s >= 1)
            def _():
                rs_copy(lane, way, s - 1, sub).wait_send()

            def add(t, _):
                sbuf[out, :, cols(t)] = (local(slot, row, t) + arr[into, :, cols(t)].astype(jnp.float32)).astype(jnp.bfloat16)
                return 0

            lax.fori_loop(0, tiles, add, 0, unroll=True)
            rs_copy(lane, way, s + 1, sub).start()
            return 0

        lax.fori_loop(0, 2, one, 0)

    def rs_last(lane, slot, chunk, half, sub):
        s = chips - 2

        def one(way, _):
            row, into = row_of(chip, way, sub), at_arr(lane, way, s, sub)
            rs_copy(lane, way, s, sub).wait_recv()
            at = pl.ds(row_of(0, way, sub), piece)

            def add(t, square):
                total = local(slot, row, t) + arr[into, :, cols(t)].astype(jnp.float32)
                new = (res[chunk, at, cols(t)].astype(jnp.float32) + total).astype(jnp.bfloat16)
                res[chunk, at, cols(t)] = new
                wide = new.astype(jnp.float32)
                return square + wide * wide

            square = lax.fori_loop(0, tiles, add, jnp.zeros((piece, WIDE), jnp.float32))
            scale = lax.rsqrt(jnp.sum(square, -1, keepdims=True) / d + EPS)

            @pl.when(half == 0)
            def _():
                def put(t, _):
                    wide = res[chunk, at, cols(t)].astype(jnp.float32)
                    bsh[lane, at, cols(t)] = (wide * scale * gm[:, cols(t)]).astype(jnp.bfloat16)
                    return 0

                lax.fori_loop(0, tiles, put, 0)

            @pl.when(half == 1)
            def _():
                def put(t, _):
                    bsh[lane, at, cols(t)] = res[chunk, at, cols(t)]
                    return 0

                lax.fori_loop(0, tiles, put, 0)

            rs_copy(lane, way, s - 1, sub).wait_send()
            return 0

        lax.fori_loop(0, 2, one, 0)

    def ag_copy(source, lane, which, there, way, s, sub):
        at = buf.at[which, pl.ds(mine + row_of(there, way, sub), piece)]
        return pltpu.make_async_remote_copy(at if source is None else source, at, ag_send.at[lane], ag_recv.at[at_arr(lane, way, s, sub)],
                                            **to(side(way)))

    def ag_over(source, lane, which, row, count):
        at = buf.at[which, pl.ds(mine + row, count)]
        return pltpu.make_async_remote_copy(at if source is None else source, at, ag_dsend.at[lane], ag_drecv.at[which], **to(partner))

    def ag_start(lane, which, sub):
        def one(way, _):
            at = bsh.at[lane, pl.ds(row_of(0, way, sub), piece)]
            row = row_of(chip, way, sub)
            ag_copy(at, lane, which, chip, way, 0, sub).start()
            ag_over(at, lane, which, row, piece).start()
            pltpu.make_async_copy(at, buf.at[which, pl.ds(mine + row, piece)], ag_loc.at[lane]).start()
            return 0

        lax.fori_loop(0, 2, one, 0)

    def ag_step(lane, which, s, sub):
        def one(way, _):
            there = place(way, s + 1)
            ag_copy(None, lane, which, there, way, s, sub).wait_recv()

            @pl.when(s < chips - 2)
            def _():
                ag_copy(None, lane, which, there, way, s + 1, sub).start()

            ag_over(None, lane, which, row_of(there, way, sub), piece).start()

            @pl.when(s == 0)
            def _():
                rs_copy(lane, way, chips - 2, sub).wait_send()

            return 0

        lax.fori_loop(0, 2, one, 0)

    def ag_came(lane, which):
        came = buf.at[which, pl.ds(theirs, half_rows)]
        pltpu.make_async_copy(came, came, ag_drecv.at[which]).wait()
        here = buf.at[which, pl.ds(mine + row_of(chip, 0, 0), share)]
        pltpu.make_async_copy(bsh.at[lane], here, ag_loc.at[lane]).wait()

    def ag_sent(lane, which):
        sent = buf.at[which, pl.ds(0, (chips - 1) * share)]
        pltpu.make_async_copy(sent, sent, ag_send.at[lane]).wait()
        over = buf.at[which, pl.ds(mine, half_rows)]
        pltpu.make_async_copy(over, over, ag_dsend.at[lane]).wait()

    def unit(lane, k):
        half, phase = lax.div(k, units // 2), lax.rem(k, 2)
        chunk = lane + 2 * lax.rem(lax.div(k, 2), chunks // 2)
        m = chunks * half + chunk
        return half, phase, chunk, m, lax.rem(m, 3)

    def lane_step(q):
        lane = lax.rem(q, 2)
        u = lax.div(q, 2) - LAG * lane

        @pl.when(u == 0)
        def _():
            rs_start(lane, unit(lane, 0)[4])

        @pl.when((u >= 1) & (u <= units * steps))
        def _():
            k, e = lax.div(u - 1, steps), lax.rem(u - 1, steps)
            half, phase, chunk, m, slot = unit(lane, k)
            s, sub = lax.div(e, SUBS), lax.rem(e, SUBS)

            @pl.when((phase == 1) & (e == AHEAD) & (k < units - 1))
            def _():
                rs_start(lane, unit(lane, k + 1)[4])

            @pl.when((phase == 0) & (s < chips - 2))
            def _():
                rs_step(lane, slot, s, sub)

            @pl.when((phase == 0) & (s == chips - 2))
            def _():
                rs_last(lane, slot, chunk, half, sub)
                ag_start(lane, m, sub)

            @pl.when((phase == 0) & (e == steps - 1) & (m + 3 < 2 * chunks))
            def _():
                pl.semaphore_signal(credit.at[slot], inc=1, **to(partner))

            @pl.when(phase == 1)
            def _():
                ag_step(lane, m, s, sub)

            @pl.when((phase == 0) & (e == 1) & (k > 0))
            def _():
                ag_sent(lane, unit(lane, k - 1)[3])

        before = 1 - lane
        v = lax.div(q + 1, 2) - 1 - LAG * before
        k = lax.div(v - 1, steps)

        @pl.when((v >= 1) & (v <= units * steps) & (lax.rem(v, steps) == 0) & (lax.rem(k, 2) == 1))
        def _():
            ag_came(before, unit(before, k)[3])

    def slots(q):
        early = a_slots
        for start, pace in ATTN:
            early += jnp.clip(lax.div((q - start) * pace, 8), 0, a_slots)
        for start, pace in MLPS:
            early += jnp.clip(lax.div((q - start) * pace, 8), 0, m_slots)
        return jnp.where(q <= 0, 0, early)

    load_act(0)
    for n in range(DEEP - 1):
        load_w1(n)
    for n in range(chunks):
        pltpu.make_async_copy(x_ref.at[n, pl.ds(mine + row_of(chip, 0, 0), share)], res.at[n], res_sem).start()

    def body(q, _):
        lax.fori_loop(slots(q), slots(q + 1), compute, 0)

        @pl.when(q == 0)
        def _():
            pltpu.make_async_copy(res, res, res_sem).wait()

        lane_step(q)
        return 0

    lax.fori_loop(0, 2 * (units * steps + LAG + 1) + 1, body, 0)
    for lane in range(2):
        ag_sent(lane, unit(lane, units - 1)[3])
    for par in range(STAGES):
        pltpu.make_async_remote_copy(stage.at[par], land.at[0, 0], st_send.at[par], d2d_recv.at[0], **to(partner)).wait_send()


def solution(mesh):
    tp = mesh.shape["tp"]

    def step(x, gain_a, wq, wk, wv, wo, gain_m, w_gate, w_up, w_down):
        chunks, rows, d = x.shape
        chips = tp // CORES
        half_rows = rows // CORES
        share = half_rows // chips
        piece = share // (2 * SUBS)
        half = HEAD // 2
        angle = jnp.arange(rows).astype(jnp.float32)[:, None] * THETA ** (-jnp.arange(half, dtype=jnp.float32) / half)
        cos, sin = jnp.cos(angle), jnp.sin(angle)
        cs, sn = jnp.concatenate([cos, cos], -1), jnp.concatenate([-sin, sin], -1)
        bf, f32 = jnp.bfloat16, jnp.float32
        vmem, dma = pltpu.VMEM, pltpu.SemaphoreType.DMA
        hbm, inside = pl.BlockSpec(memory_space=pl.ANY), pl.BlockSpec(memory_space=pltpu.VMEM)
        heads, ff = wq.shape[1] // HEAD, w_gate.shape[1]
        n_arr, n_sbuf = 2 * 2 * (chips - 1) * SUBS, 2 * 2 * 2 * SUBS
        buf = pl.pallas_call(
            functools.partial(_kernel, tp=tp),
            out_shape=jax.ShapeDtypeStruct((2 * chunks, rows, d), bf),
            in_specs=[hbm, inside, inside, inside, inside] + [hbm] * 7,
            out_specs=hbm,
            scratch_shapes=[
                vmem((rows, d), bf),
                vmem((3, d // WIDE, half_rows, WIDE), f32),
                vmem((3, d // WIDE, half_rows, WIDE), bf),
                vmem((STAGES, half_rows, WIDE), bf),
                vmem((n_arr, piece, d), bf),
                vmem((n_sbuf, piece, d), bf),
                vmem((chunks, share, d), bf),
                vmem((2, share, d), bf),
                vmem((DEEP, d, 256), bf),
                vmem((DEEP, ff, WIDE), bf),
                vmem((heads, rows, HEAD), bf),
                vmem((rows, HEAD), bf),
                vmem((rows, HEAD), bf),
                vmem((rows, heads * HEAD), bf),
                vmem((rows, ff), bf),
                vmem((rows, 256), f32),
                dma((PARTS,)), dma, dma((DEEP,)), dma((DEEP,)), dma((STAGES,)), dma((3,)), dma((n_sbuf,)), dma((n_arr,)), dma((2,)), dma((n_arr,)),
                dma((2,)), dma((2 * chunks,)), dma((2,)), pltpu.SemaphoreType.REGULAR((3,)),
            ],
            compiler_params=pltpu.CompilerParams(collective_id=0, has_side_effects=True, vmem_limit_bytes=66 * 10**6),
            name="layer",
        )(x, gain_a.astype(f32).reshape(1, d), gain_m.astype(f32).reshape(1, d), cs, sn, wq, wk, wv, wo, w_gate, w_up, w_down)
        return lax.slice_in_dim(buf, chunks, 2 * chunks, axis=0)

    tokens, whole, columns, rows_of = P("dp", None, None), P(None), P(None, "tp"), P("tp", None)
    return jax.shard_map(
        step,
        mesh=mesh,
        in_specs=(tokens, whole, columns, columns, columns, rows_of, whole, columns, columns, rows_of),
        out_specs=tokens,
        check_vma=False,
    )
```

```python
import functools
import math

import jax
import jax.numpy as jnp
from jax import lax
from jax.experimental import pallas as pl
from jax.experimental.pallas import tpu as pltpu
from jax.sharding import PartitionSpec as P

HEAD = 128
THETA = 10000
MESH = pl.DeviceIdType.MESH
HIDDEN = -1e30
LOG2E = 1.4426950408889634
CORES = 2
SUBS = 2
ATTN = (1, 8), (13, 16), (19, 8)
MLPS = (31, 16), (43, 16), (55, 16), (67, 14)
LAG = 6
DEEP = 3
STAGES = 5
M_PARTS = 2
PARTS = 4
NORM_ROWS = 64
NORM_SLOTS = 2
PAIR = 2
HOLD = 12
TAKE_ROWS = 128
BEHIND = 4
AHEAD = 3
WIDE = 512
EPS = 1e-6


def _kernel(x_ref, gain_a, gain_m, wq, wk, wv, wo, wg, wu, wd, buf, act, own, land, stage, arr, sbuf, res, bsh, w1, w2, qs, ks, vs, seen,
            hid, r256, ga, gm, cs, sn, act_sem, res_sem, w1_sem, w2_sem, st_send, d2d_recv, rs_send, rs_recv, ag_send, ag_recv, ag_dsend, ag_drecv,
            ag_loc, credit, *, tp):
    chunks, rows, d = x_ref.shape
    chips = tp // CORES
    half_rows = rows // CORES
    share = half_rows // chips
    piece = share // (2 * SUBS)
    tiles = d // WIDE
    heads = wq.shape[1] // HEAD
    ff = wg.shape[1]
    up_tiles = ff // HEAD
    q_tiles = wq.shape[1] // 256
    a_tiles = q_tiles + 1
    units = 4 * chunks // 2
    steps = (chips - 1) * SUBS
    me = lax.axis_index("tp")
    chip, core = lax.div(me, CORES), lax.rem(me, CORES)
    partner = me + 1 - 2 * core
    right, left = lax.rem(me + CORES, tp), lax.rem(me + tp - CORES, tp)
    mine = pl.multiple_of(core * half_rows, half_rows)
    theirs = pl.multiple_of((1 - core) * half_rows, half_rows)

    def to(device):
        return dict(device_id={"tp": device}, device_id_type=MESH)

    def side(way):
        return jnp.where(way == 0, right, left)

    def place(way, hops):
        return lax.rem(chip + 2 * chips + jnp.where(way == 0, -hops, hops), chips)

    barrier = pltpu.get_barrier_semaphore()
    for other in (left, right, partner):
        pl.semaphore_signal(barrier, inc=1, **to(other))

    part = rows // PARTS

    def act_copy(source, m, n):
        at = pl.ds(n * part, part)
        return pltpu.make_async_copy(source.at[lax.rem(m, chunks), at], act.at[at], act_sem.at[n])

    def load_act(m):
        @pl.when(m < chunks)
        def _():
            for n in range(PARTS):
                act_copy(x_ref, m, n).start()

        @pl.when(m >= chunks)
        def _():
            for n in range(PARTS):
                act_copy(buf, m, n).start()

    a_total = a_tiles * chunks

    def load_w1(n):
        par = lax.rem(n, DEEP)
        ja = lax.rem(n, a_tiles)

        @pl.when((n < a_total) & (ja < q_tiles))
        def _():
            pltpu.make_async_copy(wq.at[:, pl.ds(pl.multiple_of(ja * 256, 256), 256)], w1.at[par], w1_sem.at[par]).start()

        def pair(a, b, at):
            pltpu.make_async_copy(a.at[:, pl.ds(at, HEAD)], w1.at[par, :, pl.ds(0, HEAD)], w1_sem.at[par]).start()
            pltpu.make_async_copy(b.at[:, pl.ds(at, HEAD)], w1.at[par, :, pl.ds(HEAD, HEAD)], w1_sem.at[par]).start()

        @pl.when((n < a_total) & (ja == q_tiles))
        def _():
            pair(wk, wv, 0)

        @pl.when((n >= a_total) & (n < a_total + up_tiles * chunks))
        def _():
            pair(wg, wu, pl.multiple_of(lax.rem(n - a_total, up_tiles) * HEAD, HEAD))

    deep_rows = wo.shape[0]
    pack = ff // deep_rows
    groups = -(-tiles // pack)

    def w2_slot(m, j):
        first = m < chunks
        return lax.rem(jnp.where(first, groups * m + lax.div(j, pack), groups * chunks + tiles * (m - chunks) + j), DEEP)

    def wo_copy(m, j):
        at = pl.ds(pl.multiple_of(lax.rem(j, pack) * deep_rows, deep_rows), deep_rows)
        par = w2_slot(m, j)
        return pltpu.make_async_copy(wo.at[:, pl.ds(pl.multiple_of(j * WIDE, WIDE), WIDE)], w2.at[par, at], w2_sem.at[par])

    def wd_copy(m, j):
        par = w2_slot(m, j)
        return pltpu.make_async_copy(wd.at[:, pl.ds(pl.multiple_of(j * WIDE, WIDE), WIDE)], w2.at[par], w2_sem.at[par])

    def load_wo(m, group):
        def one(z, _):
            wo_copy(m, group * pack + z).start()
            return 0

        lax.fori_loop(0, jnp.minimum(pack, tiles - group * pack), one, 0)

    def norm_act(first_part):
        for n in range(first_part, first_part + PARTS // NORM_SLOTS):
            act_copy(x_ref, 0, n).wait()

            def block(r, _):
                scales, ats = [], [pl.ds(pl.multiple_of(n * part + r * NORM_ROWS + z * 16, 16), 16) for z in range(NORM_ROWS // 16)]
                for at in ats:
                    square = jnp.zeros((16, WIDE), jnp.float32)
                    for t in range(tiles):
                        wide = act[at, t * WIDE : (t + 1) * WIDE].astype(jnp.float32)
                        square += wide * wide
                    scales.append(lax.rsqrt(jnp.sum(square, -1, keepdims=True) / d + EPS))
                for at, scale in zip(ats, scales):
                    for t in range(tiles):
                        wide = act[at, t * WIDE : (t + 1) * WIDE].astype(jnp.float32)
                        act[at, t * WIDE : (t + 1) * WIDE] = (wide * scale * ga[:, t * WIDE : (t + 1) * WIDE]).astype(jnp.bfloat16)
                return 0

            lax.fori_loop(0, part // NORM_ROWS, block, 0)

    def turned(t):
        wide = t.astype(jnp.bfloat16).astype(jnp.float32)
        return (wide * cs[...] + pltpu.roll(wide, HEAD // 2, 1) * sn[...]).astype(jnp.bfloat16)

    def attention(i):
        e = HEAD**-0.5 * LOG2E
        for r in range(2):
            for z in range(PAIR):
                head = PAIR * i + z
                n, keys = rows // 2, (r + 1) * rows // 2
                q = qs[head, r * n : (r + 1) * n, :]
                s = lax.dot_general(q, ks[:keys, :], (((1,), (1,)), ((), ())), preferred_element_type=jnp.float32)
                gap = lax.broadcasted_iota(jnp.int32, s.shape, 0) + r * n - lax.broadcasted_iota(jnp.int32, s.shape, 1)
                s = jnp.where(gap >= 0, s, HIDDEN)
                p = jnp.exp2((s - s.max(-1, keepdims=True)) * e)
                o = jnp.dot(p.astype(jnp.bfloat16), vs[:keys, :], preferred_element_type=jnp.float32)
                o = o * (1 / p.sum(-1, keepdims=True))
                seen[r * n : (r + 1) * n, pl.ds(pl.multiple_of(head * HEAD, HEAD), HEAD)] = o.astype(jnp.bfloat16)

    b_slots = NORM_SLOTS + a_tiles
    a_slots, m_slots = b_slots + heads // PAIR + tiles // 2, up_tiles + tiles

    def compute(g, _):
        first = g < a_slots * chunks
        after = g - a_slots * chunks
        m = jnp.where(first, lax.div(g, a_slots), chunks + lax.div(after, m_slots))
        i = jnp.where(first, lax.rem(g, a_slots), lax.rem(after, m_slots))
        slot = lax.rem(m, 3)

        for n in range(NORM_SLOTS):

            @pl.when((i == n) & first)
            def _():
                norm_act(n * (PARTS // NORM_SLOTS))

        @pl.when((i == 0) & jnp.logical_not(first))
        def _():
            for n in range(PARTS):
                act_copy(buf, 0, n).wait()

        def tile1(n):
            par = lax.rem(n, DEEP)
            pltpu.make_async_copy(w1.at[par], w1.at[par], w1_sem.at[par]).wait()
            load_w1(n + DEEP - 1)
            return par

        @pl.when(first & (i >= NORM_SLOTS) & (i < b_slots))
        def _():
            j = i - NORM_SLOTS
            par = tile1(a_tiles * m + j)
            r256[...] = jnp.dot(act[...], w1[par], preferred_element_type=jnp.float32)

            @pl.when(j < q_tiles)
            def _():
                qs[2 * j] = turned(r256[:, :HEAD])
                qs[2 * j + 1] = turned(r256[:, HEAD:])

            @pl.when(j == q_tiles)
            def _():
                ks[...] = turned(r256[:, :HEAD])
                vs[...] = r256[:, HEAD:].astype(jnp.bfloat16)

        @pl.when(jnp.logical_not(first) & (i < up_tiles))
        def _():
            par = tile1(a_total + up_tiles * (m - chunks) + i)
            at = pl.ds(pl.multiple_of(i * HEAD, HEAD), HEAD)
            for r in range(0, rows, rows // M_PARTS):
                both = jnp.dot(act[r : r + rows // M_PARTS, :], w1[par], preferred_element_type=jnp.float32)
                hid[r : r + rows // M_PARTS, at] = (jax.nn.silu(both[:, :HEAD]) * both[:, HEAD:]).astype(jnp.bfloat16)

        @pl.when(first & (i >= b_slots) & (i < b_slots + heads // PAIR))
        def _():
            attention(i - b_slots)

        @pl.when(i == 3)
        def _():
            @pl.when(first)
            def _():
                for n in range(DEEP):
                    load_wo(m, n)

            @pl.when(jnp.logical_not(first))
            def _():
                for j in range(DEEP - 1):
                    wd_copy(m, j).start()

        last = jnp.where(first, b_slots + heads // PAIR, up_tiles)

        ahead = jnp.where(m < chunks - 1, last, jnp.where(m == chunks - 1, a_slots - 1, m_slots - 2))

        @pl.when((i == ahead) & (m < 2 * chunks - 1))
        def _():
            load_act(m + 1)

        @pl.when((i == last) & (m >= 3))
        def _():
            pl.semaphore_wait(credit.at[slot], 1)

        def put(j, source, weights):
            out = lax.rem(j, STAGES)
            copy = pltpu.make_async_remote_copy(stage.at[out], land.at[slot, j], st_send.at[out], d2d_recv.at[slot], **to(partner))

            @pl.when(m * tiles + j >= STAGES)
            def _():
                copy.wait_send()

            stage[out] = jnp.dot(source[pl.ds(theirs, half_rows), :], weights, preferred_element_type=jnp.float32).astype(jnp.bfloat16)
            copy.start()
            own[slot, j] = jnp.dot(source[pl.ds(mine, half_rows), :], weights, preferred_element_type=jnp.float32)

        @pl.when(first & (i >= last))
        def _():
            def tile2(jj, _):
                j = 2 * (i - last) + jj
                par = w2_slot(m, j)

                @pl.when(lax.rem(j, pack) == 0)
                def _():
                    def one(z, _):
                        wo_copy(m, j).wait()
                        return 0

                    lax.fori_loop(0, jnp.minimum(pack, tiles - j), one, 0)

                put(j, seen, w2[par, pl.ds(pl.multiple_of(lax.rem(j, pack) * deep_rows, deep_rows), deep_rows), :])

                @pl.when(j == pack - 1)
                def _():
                    for n in range(DEEP, groups):
                        load_wo(m, n)

                return 0

            lax.fori_loop(0, 2, tile2, 0)

        @pl.when(jnp.logical_not(first) & (i >= last))
        def _():
            j = i - last
            wd_copy(m, j).wait()

            @pl.when(j + DEEP - 1 < tiles)
            def _():
                wd_copy(m, j + DEEP - 1).start()

            put(j, hid, w2[w2_slot(m, j)])

        return 0

    def at_arr(lane, way, s, sub):
        return ((lane * 2 + way) * (chips - 1) + s) * SUBS + sub

    def at_sbuf(lane, way, s, sub):
        return ((lane * 2 + way) * 2 + lax.rem(s, 2)) * SUBS + sub

    def row_of(there, way, sub):
        return pl.multiple_of(there * share + way * (share // 2) + sub * piece, piece)

    def rs_copy(lane, way, s, sub):
        return pltpu.make_async_remote_copy(
            sbuf.at[at_sbuf(lane, way, s, sub)], arr.at[at_arr(lane, way, s, sub)], rs_send.at[at_sbuf(lane, way, s, sub)],
            rs_recv.at[at_arr(lane, way, s, sub)], **to(side(way)))

    def cols(t):
        return pl.ds(pl.multiple_of(t * WIDE, WIDE), WIDE)

    def local(slot, row, t):
        at = pl.ds(row, piece)
        return own[slot, t, at, :] + land[slot, t, at, :].astype(jnp.float32)

    def rs_start(lane, slot):
        pltpu.make_async_copy(land.at[slot], land.at[slot], d2d_recv.at[slot]).wait()

        def one(z, _):
            sub, way = lax.div(z, 2), lax.rem(z, 2)
            row, out = row_of(place(way, 1), way, sub), at_sbuf(lane, way, 0, sub)

            def add(t, _):
                sbuf[out, :, cols(t)] = local(slot, row, t).astype(jnp.bfloat16)
                return 0

            lax.fori_loop(0, tiles, add, 0, unroll=True)
            rs_copy(lane, way, 0, sub).start()
            return 0

        lax.fori_loop(0, 2 * SUBS, one, 0)

    def rs_step(lane, slot, s, sub):
        def one(way, _):
            row, out, into = row_of(place(way, s + 2), way, sub), at_sbuf(lane, way, s + 1, sub), at_arr(lane, way, s, sub)
            rs_copy(lane, way, s, sub).wait_recv()

            @pl.when(s >= 1)
            def _():
                rs_copy(lane, way, s - 1, sub).wait_send()

            def add(t, _):
                sbuf[out, :, cols(t)] = (local(slot, row, t) + arr[into, :, cols(t)].astype(jnp.float32)).astype(jnp.bfloat16)
                return 0

            lax.fori_loop(0, tiles, add, 0, unroll=True)
            rs_copy(lane, way, s + 1, sub).start()
            return 0

        lax.fori_loop(0, 2, one, 0)

    def rs_last(lane, slot, chunk, half, sub):
        s = chips - 2

        def one(way, _):
            row, into = row_of(chip, way, sub), at_arr(lane, way, s, sub)
            rs_copy(lane, way, s, sub).wait_recv()
            at = pl.ds(row_of(0, way, sub), piece)

            def add(t, square):
                total = local(slot, row, t) + arr[into, :, cols(t)].astype(jnp.float32)
                new = (res[chunk, at, cols(t)].astype(jnp.float32) + total).astype(jnp.bfloat16)
                res[chunk, at, cols(t)] = new
                wide = new.astype(jnp.float32)
                return square + wide * wide

            square = lax.fori_loop(0, tiles, add, jnp.zeros((piece, WIDE), jnp.float32))
            scale = lax.rsqrt(jnp.sum(square, -1, keepdims=True) / d + EPS)

            @pl.when(half == 0)
            def _():
                def put(t, _):
                    wide = res[chunk, at, cols(t)].astype(jnp.float32)
                    bsh[lane, at, cols(t)] = (wide * scale * gm[:, cols(t)]).astype(jnp.bfloat16)
                    return 0

                lax.fori_loop(0, tiles, put, 0)

            @pl.when(half == 1)
            def _():
                def put(t, _):
                    bsh[lane, at, cols(t)] = res[chunk, at, cols(t)]
                    return 0

                lax.fori_loop(0, tiles, put, 0)

            rs_copy(lane, way, s - 1, sub).wait_send()
            return 0

        lax.fori_loop(0, 2, one, 0)

    def ag_copy(source, lane, which, there, way, s, sub):
        at = buf.at[which, pl.ds(mine + row_of(there, way, sub), piece)]
        return pltpu.make_async_remote_copy(at if source is None else source, at, ag_send.at[lane], ag_recv.at[at_arr(lane, way, s, sub)],
                                            **to(side(way)))

    def ag_over(source, lane, which, row, count):
        at = buf.at[which, pl.ds(mine + row, count)]
        return pltpu.make_async_remote_copy(at if source is None else source, at, ag_dsend.at[lane], ag_drecv.at[which], **to(partner))

    def ag_start(lane, which, sub):
        def one(way, _):
            at = bsh.at[lane, pl.ds(row_of(0, way, sub), piece)]
            row = row_of(chip, way, sub)
            ag_copy(at, lane, which, chip, way, 0, sub).start()
            ag_over(at, lane, which, row, piece).start()
            pltpu.make_async_copy(at, buf.at[which, pl.ds(mine + row, piece)], ag_loc.at[lane]).start()
            return 0

        lax.fori_loop(0, 2, one, 0)

    def ag_step(lane, which, s, sub):
        def one(way, _):
            there = place(way, s + 1)
            ag_copy(None, lane, which, there, way, s, sub).wait_recv()

            @pl.when(s < chips - 2)
            def _():
                ag_copy(None, lane, which, there, way, s + 1, sub).start()

            ag_over(None, lane, which, row_of(there, way, sub), piece).start()

            @pl.when(s == 0)
            def _():
                rs_copy(lane, way, chips - 2, sub).wait_send()

            return 0

        lax.fori_loop(0, 2, one, 0)

    def ag_came(lane, which):
        came = buf.at[which, pl.ds(theirs, half_rows)]
        pltpu.make_async_copy(came, came, ag_drecv.at[which]).wait()
        here = buf.at[which, pl.ds(mine + row_of(chip, 0, 0), share)]
        pltpu.make_async_copy(bsh.at[lane], here, ag_loc.at[lane]).wait()

    def ag_sent(lane, which):
        sent = buf.at[which, pl.ds(0, (chips - 1) * share)]
        pltpu.make_async_copy(sent, sent, ag_send.at[lane]).wait()
        over = buf.at[which, pl.ds(mine, half_rows)]
        pltpu.make_async_copy(over, over, ag_dsend.at[lane]).wait()

    def unit(lane, k):
        half, phase = lax.div(k, units // 2), lax.rem(k, 2)
        chunk = lane + 2 * lax.rem(lax.div(k, 2), chunks // 2)
        m = chunks * half + chunk
        return half, phase, chunk, m, lax.rem(m, 3)

    def lane_step(q):
        lane = lax.rem(q, 2)
        u = lax.div(q, 2) - LAG * lane

        @pl.when(u == 0)
        def _():
            rs_start(lane, unit(lane, 0)[4])

        @pl.when((u >= 1) & (u <= units * steps))
        def _():
            k, e = lax.div(u - 1, steps), lax.rem(u - 1, steps)
            half, phase, chunk, m, slot = unit(lane, k)
            s, sub = lax.div(e, SUBS), lax.rem(e, SUBS)

            @pl.when((phase == 1) & (e == AHEAD) & (k < units - 1))
            def _():
                rs_start(lane, unit(lane, k + 1)[4])

            @pl.when((phase == 0) & (s < chips - 2))
            def _():
                rs_step(lane, slot, s, sub)

            @pl.when((phase == 0) & (s == chips - 2))
            def _():
                rs_last(lane, slot, chunk, half, sub)
                ag_start(lane, m, sub)

            @pl.when((phase == 0) & (e == steps - 1) & (m + 3 < 2 * chunks))
            def _():
                pl.semaphore_signal(credit.at[slot], inc=1, **to(partner))

            @pl.when(phase == 1)
            def _():
                ag_step(lane, m, s, sub)

            @pl.when((phase == 0) & (e == 1) & (k > 0))
            def _():
                ag_sent(lane, unit(lane, k - 1)[3])

        before = 1 - lane
        v = lax.div(q + 1, 2) - 1 - LAG * before
        k = lax.div(v - 1, steps)

        @pl.when((v >= 1) & (v <= units * steps) & (lax.rem(v, steps) == 0) & (lax.rem(k, 2) == 1))
        def _():
            ag_came(before, unit(before, k)[3])

    def slots(q):
        early = a_slots
        for start, pace in ATTN:
            early += jnp.clip(lax.div((q - start) * pace, 8), 0, a_slots)
        for start, pace in MLPS:
            early += jnp.clip(lax.div((q - start) * pace, 8), 0, m_slots)
        return jnp.where(q <= 0, 0, early)

    load_act(0)
    for n in range(DEEP - 1):
        load_w1(n)
    for n in range(chunks):
        pltpu.make_async_copy(x_ref.at[n, pl.ds(mine + row_of(chip, 0, 0), share)], res.at[n], res_sem).start()
    ga[...] = gain_a[...].astype(jnp.float32).reshape(1, d)
    gm[...] = gain_m[...].astype(jnp.float32).reshape(1, d)
    half = HEAD // 2
    pair = lax.rem(lax.broadcasted_iota(jnp.int32, (1, HEAD), 1), half).astype(jnp.float32)
    sign = jnp.where(lax.broadcasted_iota(jnp.int32, (1, HEAD), 1) < half, -1.0, 1.0)
    speed = jnp.exp(pair * (-math.log(THETA) / half))

    def table(r, _):
        at = pl.ds(pl.multiple_of(r * 64, 64), 64)
        angle = (lax.broadcasted_iota(jnp.int32, (64, HEAD), 0) + r * 64).astype(jnp.float32) * speed
        cs[at, :] = jnp.cos(angle)
        sn[at, :] = jnp.sin(angle) * sign
        return 0

    lax.fori_loop(0, rows // 64, table, 0)
    pl.semaphore_wait(barrier, 3)

    def body(q, _):
        lax.fori_loop(slots(q), slots(q + 1), compute, 0)

        @pl.when(q == 0)
        def _():
            pltpu.make_async_copy(res, res, res_sem).wait()

        lane_step(q)
        return 0

    lax.fori_loop(0, 2 * (units * steps + LAG + 1) + 1, body, 0)
    for lane in range(2):
        ag_sent(lane, unit(lane, units - 1)[3])
    for par in range(STAGES):
        pltpu.make_async_remote_copy(stage.at[par], land.at[0, 0], st_send.at[par], d2d_recv.at[0], **to(partner)).wait_send()


def _take(buf, y, hold, came, left):
    chunks, rows, _ = y.shape
    deep, block, _ = hold.shape
    each = rows // block
    total = chunks * each

    def copies(n):
        c, at, z = n // each, pl.ds(n % each * block, block), n % deep
        return (pltpu.make_async_copy(buf.at[chunks + c, at], hold.at[z], came.at[z]),
                pltpu.make_async_copy(hold.at[z], y.at[c, at], left.at[z]))

    for n in range(min(deep, total)):
        copies(n)[0].start()
    for n in range(total):
        copies(n)[0].wait()
        copies(n)[1].start()
        if n >= BEHIND and n - BEHIND + deep < total:
            copies(n - BEHIND)[1].wait()
            copies(n - BEHIND + deep)[0].start()
    for n in range(max(total - deep, 0), total):
        copies(n)[1].wait()


def solution(mesh):
    tp = mesh.shape["tp"]

    def step(x, gain_a, wq, wk, wv, wo, gain_m, w_gate, w_up, w_down):
        chunks, rows, d = x.shape
        chips = tp // CORES
        half_rows = rows // CORES
        share = half_rows // chips
        piece = share // (2 * SUBS)
        bf, f32 = jnp.bfloat16, jnp.float32
        vmem, dma = pltpu.VMEM, pltpu.SemaphoreType.DMA
        hbm, inside = pl.BlockSpec(memory_space=pl.ANY), pl.BlockSpec(memory_space=pltpu.VMEM)
        heads, ff = wq.shape[1] // HEAD, w_gate.shape[1]
        n_arr, n_sbuf = 2 * 2 * (chips - 1) * SUBS, 2 * 2 * 2 * SUBS
        buf = pl.pallas_call(
            functools.partial(_kernel, tp=tp),
            out_shape=jax.ShapeDtypeStruct((2 * chunks, rows, d), bf),
            in_specs=[hbm, inside, inside] + [hbm] * 7,
            out_specs=hbm,
            scratch_shapes=[
                vmem((rows, d), bf),
                vmem((3, d // WIDE, half_rows, WIDE), f32),
                vmem((3, d // WIDE, half_rows, WIDE), bf),
                vmem((STAGES, half_rows, WIDE), bf),
                vmem((n_arr, piece, d), bf),
                vmem((n_sbuf, piece, d), bf),
                vmem((chunks, share, d), bf),
                vmem((2, share, d), bf),
                vmem((DEEP, d, 256), bf),
                vmem((DEEP, ff, WIDE), bf),
                vmem((heads, rows, HEAD), bf),
                vmem((rows, HEAD), bf),
                vmem((rows, HEAD), bf),
                vmem((rows, heads * HEAD), bf),
                vmem((rows, ff), bf),
                vmem((rows, 256), f32),
                vmem((1, d), f32),
                vmem((1, d), f32),
                vmem((rows, HEAD), f32),
                vmem((rows, HEAD), f32),
                dma((PARTS,)), dma, dma((DEEP,)), dma((DEEP,)), dma((STAGES,)), dma((3,)), dma((n_sbuf,)), dma((n_arr,)), dma((2,)), dma((n_arr,)),
                dma((2,)), dma((2 * chunks,)), dma((2,)), pltpu.SemaphoreType.REGULAR((3,)),
            ],
            compiler_params=pltpu.CompilerParams(collective_id=0, has_side_effects=True, vmem_limit_bytes=66 * 10**6),
            name="layer",
        )(x, gain_a, gain_m, wq, wk, wv, wo, w_gate, w_up, w_down)
        return pl.pallas_call(
            _take,
            out_shape=jax.ShapeDtypeStruct(x.shape, bf),
            in_specs=[hbm],
            out_specs=hbm,
            scratch_shapes=[vmem((HOLD, TAKE_ROWS, d), bf), dma((HOLD,)), dma((HOLD,))],
            compiler_params=pltpu.CompilerParams(vmem_limit_bytes=66 * 10**6),
            name="take",
        )(buf)

    tokens, whole, columns, rows_of = P("dp", None, None), P(None), P(None, "tp"), P("tp", None)
    return jax.shard_map(
        step,
        mesh=mesh,
        in_specs=(tokens, whole, columns, columns, columns, rows_of, whole, columns, columns, rows_of),
        out_specs=tokens,
        check_vma=False,
    )
```

```python
import functools
import math

import jax
import jax.numpy as jnp
from jax import lax
from jax.experimental import pallas as pl
from jax.experimental.pallas import tpu as pltpu
from jax.sharding import PartitionSpec as P

HEAD = 128
THETA = 10000
MESH = pl.DeviceIdType.MESH
HIDDEN = -1e30
LOG2E = 1.4426950408889634
CORES = 2
SUBS = 2
ATTN = (1, 8), (13, 16), (19, 8)
MLPS = (31, 16), (43, 16), (55, 16), (67, 14)
LAG = 6
DEEP = 3
STAGES = 5
M_PARTS = 2
PARTS = 4
NORM_ROWS = 64
NORM_SLOTS = 2
PAIR = 4
HOLD = 12
TAKE_ROWS = 128
BEHIND = 4
AHEAD = 3
WIDE = 512
EPS = 1e-6


def _kernel(x_ref, gain_a, gain_m, wq, wk, wv, wo, wg, wu, wd, buf, act, own, land, stage, arr, sbuf, res, bsh, w1, w2, qs, ks, vs, seen,
            hid, r256, ga, gm, cs, sn, act_sem, res_sem, w1_sem, w2_sem, st_send, d2d_recv, rs_send, rs_recv, ag_send, ag_recv, ag_dsend, ag_drecv,
            ag_loc, credit, *, tp):
    chunks, rows, d = x_ref.shape
    chips = tp // CORES
    half_rows = rows // CORES
    share = half_rows // chips
    piece = share // (2 * SUBS)
    tiles = d // WIDE
    heads = wq.shape[1] // HEAD
    ff = wg.shape[1]
    up_tiles = ff // HEAD
    q_tiles = wq.shape[1] // 256
    a_tiles = q_tiles + 1
    units = 4 * chunks // 2
    steps = (chips - 1) * SUBS
    me = lax.axis_index("tp")
    chip, core = lax.div(me, CORES), lax.rem(me, CORES)
    partner = me + 1 - 2 * core
    right, left = lax.rem(me + CORES, tp), lax.rem(me + tp - CORES, tp)
    mine = pl.multiple_of(core * half_rows, half_rows)
    theirs = pl.multiple_of((1 - core) * half_rows, half_rows)

    def to(device):
        return dict(device_id={"tp": device}, device_id_type=MESH)

    def side(way):
        return jnp.where(way == 0, right, left)

    def place(way, hops):
        return lax.rem(chip + 2 * chips + jnp.where(way == 0, -hops, hops), chips)

    barrier = pltpu.get_barrier_semaphore()
    for other in (left, right, partner):
        pl.semaphore_signal(barrier, inc=1, **to(other))

    part = rows // PARTS

    def act_copy(source, m, n):
        at = pl.ds(n * part, part)
        return pltpu.make_async_copy(source.at[lax.rem(m, chunks), at], act.at[at], act_sem.at[n])

    def load_act(m):
        @pl.when(m < chunks)
        def _():
            for n in range(PARTS):
                act_copy(x_ref, m, n).start()

        @pl.when(m >= chunks)
        def _():
            for n in range(PARTS):
                act_copy(buf, m, n).start()

    a_total = a_tiles * chunks

    def load_w1(n):
        par = lax.rem(n, DEEP)
        ja = lax.rem(n, a_tiles)

        @pl.when((n < a_total) & (ja < q_tiles))
        def _():
            pltpu.make_async_copy(wq.at[:, pl.ds(pl.multiple_of(ja * 256, 256), 256)], w1.at[par], w1_sem.at[par]).start()

        def pair(a, b, at):
            pltpu.make_async_copy(a.at[:, pl.ds(at, HEAD)], w1.at[par, :, pl.ds(0, HEAD)], w1_sem.at[par]).start()
            pltpu.make_async_copy(b.at[:, pl.ds(at, HEAD)], w1.at[par, :, pl.ds(HEAD, HEAD)], w1_sem.at[par]).start()

        @pl.when((n < a_total) & (ja == q_tiles))
        def _():
            pair(wk, wv, 0)

        @pl.when((n >= a_total) & (n < a_total + up_tiles * chunks))
        def _():
            pair(wg, wu, pl.multiple_of(lax.rem(n - a_total, up_tiles) * HEAD, HEAD))

    deep_rows = wo.shape[0]
    pack = ff // deep_rows
    groups = -(-tiles // pack)

    def w2_slot(m, j):
        first = m < chunks
        return lax.rem(jnp.where(first, groups * m + lax.div(j, pack), groups * chunks + tiles * (m - chunks) + j), DEEP)

    def wo_copy(m, j):
        at = pl.ds(pl.multiple_of(lax.rem(j, pack) * deep_rows, deep_rows), deep_rows)
        par = w2_slot(m, j)
        return pltpu.make_async_copy(wo.at[:, pl.ds(pl.multiple_of(j * WIDE, WIDE), WIDE)], w2.at[par, at], w2_sem.at[par])

    def wd_copy(m, j):
        par = w2_slot(m, j)
        return pltpu.make_async_copy(wd.at[:, pl.ds(pl.multiple_of(j * WIDE, WIDE), WIDE)], w2.at[par], w2_sem.at[par])

    def load_wo(m, group):
        def one(z, _):
            wo_copy(m, group * pack + z).start()
            return 0

        lax.fori_loop(0, jnp.minimum(pack, tiles - group * pack), one, 0)

    def norm_act(first_part):
        for n in range(first_part, first_part + PARTS // NORM_SLOTS):
            act_copy(x_ref, 0, n).wait()

            def block(r, _):
                scales, ats = [], [pl.ds(pl.multiple_of(n * part + r * NORM_ROWS + z * 16, 16), 16) for z in range(NORM_ROWS // 16)]
                for at in ats:
                    square = jnp.zeros((16, WIDE), jnp.float32)
                    for t in range(tiles):
                        wide = act[at, t * WIDE : (t + 1) * WIDE].astype(jnp.float32)
                        square += wide * wide
                    scales.append(lax.rsqrt(jnp.sum(square, -1, keepdims=True) / d + EPS))
                for at, scale in zip(ats, scales):
                    for t in range(tiles):
                        wide = act[at, t * WIDE : (t + 1) * WIDE].astype(jnp.float32)
                        act[at, t * WIDE : (t + 1) * WIDE] = (wide * scale * ga[:, t * WIDE : (t + 1) * WIDE]).astype(jnp.bfloat16)
                return 0

            lax.fori_loop(0, part // NORM_ROWS, block, 0)

    def turned(t):
        wide = t.astype(jnp.bfloat16).astype(jnp.float32)
        return (wide * cs[...] + pltpu.roll(wide, HEAD // 2, 1) * sn[...]).astype(jnp.bfloat16)

    def attention(i):
        e = HEAD**-0.5 * LOG2E
        for r in range(2):
            for z in range(PAIR):
                head = PAIR * i + z
                n, keys = rows // 2, (r + 1) * rows // 2
                q = qs[head, r * n : (r + 1) * n, :]
                s = lax.dot_general(q, ks[:keys, :], (((1,), (1,)), ((), ())), preferred_element_type=jnp.float32)
                gap = lax.broadcasted_iota(jnp.int32, s.shape, 0) + r * n - lax.broadcasted_iota(jnp.int32, s.shape, 1)
                s = jnp.where(gap >= 0, s, HIDDEN)
                p = jnp.exp2((s - s.max(-1, keepdims=True)) * e)
                o = jnp.dot(p.astype(jnp.bfloat16), vs[:keys, :], preferred_element_type=jnp.float32)
                o = o * (1 / p.sum(-1, keepdims=True))
                seen[r * n : (r + 1) * n, pl.ds(pl.multiple_of(head * HEAD, HEAD), HEAD)] = o.astype(jnp.bfloat16)

    b_slots = NORM_SLOTS + a_tiles
    a_slots, m_slots = b_slots + heads // PAIR + tiles // 2, up_tiles + tiles

    def compute(g, _):
        first = g < a_slots * chunks
        after = g - a_slots * chunks
        m = jnp.where(first, lax.div(g, a_slots), chunks + lax.div(after, m_slots))
        i = jnp.where(first, lax.rem(g, a_slots), lax.rem(after, m_slots))
        slot = lax.rem(m, 3)

        @pl.when(g == NORM_SLOTS - 1)
        def _():
            for n in range(1, DEEP - 1):
                load_w1(n)

        for n in range(NORM_SLOTS):

            @pl.when((i == n) & first)
            def _():
                norm_act(n * (PARTS // NORM_SLOTS))

        @pl.when((i == 0) & jnp.logical_not(first))
        def _():
            for n in range(PARTS):
                act_copy(buf, 0, n).wait()

        def tile1(n):
            par = lax.rem(n, DEEP)
            pltpu.make_async_copy(w1.at[par], w1.at[par], w1_sem.at[par]).wait()
            load_w1(n + DEEP - 1)
            return par

        @pl.when(first & (i >= NORM_SLOTS) & (i < b_slots))
        def _():
            j = i - NORM_SLOTS
            par = tile1(a_tiles * m + j)
            r256[...] = jnp.dot(act[...], w1[par], preferred_element_type=jnp.float32)

            @pl.when(j < q_tiles)
            def _():
                qs[2 * j] = turned(r256[:, :HEAD])
                qs[2 * j + 1] = turned(r256[:, HEAD:])

            @pl.when(j == q_tiles)
            def _():
                ks[...] = turned(r256[:, :HEAD])
                vs[...] = r256[:, HEAD:].astype(jnp.bfloat16)

        @pl.when(jnp.logical_not(first) & (i < up_tiles))
        def _():
            par = tile1(a_total + up_tiles * (m - chunks) + i)
            at = pl.ds(pl.multiple_of(i * HEAD, HEAD), HEAD)
            for r in range(0, rows, rows // M_PARTS):
                both = jnp.dot(act[r : r + rows // M_PARTS, :], w1[par], preferred_element_type=jnp.float32)
                hid[r : r + rows // M_PARTS, at] = (jax.nn.silu(both[:, :HEAD]) * both[:, HEAD:]).astype(jnp.bfloat16)

        @pl.when(first & (i >= b_slots) & (i < b_slots + heads // PAIR))
        def _():
            attention(i - b_slots)

        @pl.when(i == 3)
        def _():
            @pl.when(first)
            def _():
                for n in range(DEEP):
                    load_wo(m, n)

            @pl.when(jnp.logical_not(first))
            def _():
                for j in range(DEEP - 1):
                    wd_copy(m, j).start()

        last = jnp.where(first, b_slots + heads // PAIR, up_tiles)

        ahead = jnp.where(m < chunks - 1, last, jnp.where(m == chunks - 1, a_slots - 1, m_slots - 2))

        @pl.when((i == ahead) & (m < 2 * chunks - 1))
        def _():
            load_act(m + 1)

        @pl.when((i == last) & (m >= 3))
        def _():
            pl.semaphore_wait(credit.at[slot], 1)

        def put(j, source, weights):
            out = lax.rem(j, STAGES)
            copy = pltpu.make_async_remote_copy(stage.at[out], land.at[slot, j], st_send.at[out], d2d_recv.at[slot], **to(partner))

            @pl.when(m * tiles + j >= STAGES)
            def _():
                copy.wait_send()

            stage[out] = jnp.dot(source[pl.ds(theirs, half_rows), :], weights, preferred_element_type=jnp.float32).astype(jnp.bfloat16)
            copy.start()
            own[slot, j] = jnp.dot(source[pl.ds(mine, half_rows), :], weights, preferred_element_type=jnp.float32)

        @pl.when(first & (i >= last))
        def _():
            def tile2(jj, _):
                j = 2 * (i - last) + jj
                par = w2_slot(m, j)

                @pl.when(lax.rem(j, pack) == 0)
                def _():
                    def one(z, _):
                        wo_copy(m, j).wait()
                        return 0

                    lax.fori_loop(0, jnp.minimum(pack, tiles - j), one, 0)

                put(j, seen, w2[par, pl.ds(pl.multiple_of(lax.rem(j, pack) * deep_rows, deep_rows), deep_rows), :])

                @pl.when(j == pack - 1)
                def _():
                    for n in range(DEEP, groups):
                        load_wo(m, n)

                return 0

            lax.fori_loop(0, 2, tile2, 0)

        @pl.when(jnp.logical_not(first) & (i >= last))
        def _():
            j = i - last
            wd_copy(m, j).wait()

            @pl.when(j + DEEP - 1 < tiles)
            def _():
                wd_copy(m, j + DEEP - 1).start()

            put(j, hid, w2[w2_slot(m, j)])

        return 0

    def at_arr(lane, way, s, sub):
        return ((lane * 2 + way) * (chips - 1) + s) * SUBS + sub

    def at_sbuf(lane, way, s, sub):
        return ((lane * 2 + way) * 2 + lax.rem(s, 2)) * SUBS + sub

    def row_of(there, way, sub):
        return pl.multiple_of(there * share + way * (share // 2) + sub * piece, piece)

    def rs_copy(lane, way, s, sub):
        return pltpu.make_async_remote_copy(
            sbuf.at[at_sbuf(lane, way, s, sub)], arr.at[at_arr(lane, way, s, sub)], rs_send.at[at_sbuf(lane, way, s, sub)],
            rs_recv.at[at_arr(lane, way, s, sub)], **to(side(way)))

    def cols(t):
        return pl.ds(pl.multiple_of(t * WIDE, WIDE), WIDE)

    def local(slot, row, t):
        at = pl.ds(row, piece)
        return own[slot, t, at, :] + land[slot, t, at, :].astype(jnp.float32)

    def rs_start(lane, slot):
        pltpu.make_async_copy(land.at[slot], land.at[slot], d2d_recv.at[slot]).wait()

        def one(z, _):
            sub, way = lax.div(z, 2), lax.rem(z, 2)
            row, out = row_of(place(way, 1), way, sub), at_sbuf(lane, way, 0, sub)

            def add(t, _):
                sbuf[out, :, cols(t)] = local(slot, row, t).astype(jnp.bfloat16)
                return 0

            lax.fori_loop(0, tiles, add, 0, unroll=True)
            rs_copy(lane, way, 0, sub).start()
            return 0

        lax.fori_loop(0, 2 * SUBS, one, 0)

    def rs_step(lane, slot, s, sub):
        def one(way, _):
            row, out, into = row_of(place(way, s + 2), way, sub), at_sbuf(lane, way, s + 1, sub), at_arr(lane, way, s, sub)
            rs_copy(lane, way, s, sub).wait_recv()

            @pl.when(s >= 1)
            def _():
                rs_copy(lane, way, s - 1, sub).wait_send()

            def add(t, _):
                sbuf[out, :, cols(t)] = (local(slot, row, t) + arr[into, :, cols(t)].astype(jnp.float32)).astype(jnp.bfloat16)
                return 0

            lax.fori_loop(0, tiles, add, 0, unroll=True)
            rs_copy(lane, way, s + 1, sub).start()
            return 0

        lax.fori_loop(0, 2, one, 0)

    def rs_last(lane, slot, chunk, half, sub):
        s = chips - 2

        def one(way, _):
            row, into = row_of(chip, way, sub), at_arr(lane, way, s, sub)
            rs_copy(lane, way, s, sub).wait_recv()
            at = pl.ds(row_of(0, way, sub), piece)

            def add(t, square):
                total = local(slot, row, t) + arr[into, :, cols(t)].astype(jnp.float32)
                new = (res[chunk, at, cols(t)].astype(jnp.float32) + total).astype(jnp.bfloat16)
                res[chunk, at, cols(t)] = new
                wide = new.astype(jnp.float32)
                return square + wide * wide

            square = lax.fori_loop(0, tiles, add, jnp.zeros((piece, WIDE), jnp.float32))
            scale = lax.rsqrt(jnp.sum(square, -1, keepdims=True) / d + EPS)

            @pl.when(half == 0)
            def _():
                def put(t, _):
                    wide = res[chunk, at, cols(t)].astype(jnp.float32)
                    bsh[lane, at, cols(t)] = (wide * scale * gm[:, cols(t)]).astype(jnp.bfloat16)
                    return 0

                lax.fori_loop(0, tiles, put, 0)

            @pl.when(half == 1)
            def _():
                def put(t, _):
                    bsh[lane, at, cols(t)] = res[chunk, at, cols(t)]
                    return 0

                lax.fori_loop(0, tiles, put, 0)

            rs_copy(lane, way, s - 1, sub).wait_send()
            return 0

        lax.fori_loop(0, 2, one, 0)

    def ag_copy(source, lane, which, there, way, s, sub):
        at = buf.at[which, pl.ds(mine + row_of(there, way, sub), piece)]
        return pltpu.make_async_remote_copy(at if source is None else source, at, ag_send.at[lane], ag_recv.at[at_arr(lane, way, s, sub)],
                                            **to(side(way)))

    def ag_over(source, lane, which, row, count):
        at = buf.at[which, pl.ds(mine + row, count)]
        return pltpu.make_async_remote_copy(at if source is None else source, at, ag_dsend.at[lane], ag_drecv.at[which], **to(partner))

    def ag_start(lane, which, sub):
        def one(way, _):
            at = bsh.at[lane, pl.ds(row_of(0, way, sub), piece)]
            row = row_of(chip, way, sub)
            ag_copy(at, lane, which, chip, way, 0, sub).start()
            ag_over(at, lane, which, row, piece).start()
            pltpu.make_async_copy(at, buf.at[which, pl.ds(mine + row, piece)], ag_loc.at[lane]).start()
            return 0

        lax.fori_loop(0, 2, one, 0)

    def ag_step(lane, which, s, sub):
        def one(way, _):
            there = place(way, s + 1)
            ag_copy(None, lane, which, there, way, s, sub).wait_recv()

            @pl.when(s < chips - 2)
            def _():
                ag_copy(None, lane, which, there, way, s + 1, sub).start()

            ag_over(None, lane, which, row_of(there, way, sub), piece).start()

            @pl.when(s == 0)
            def _():
                rs_copy(lane, way, chips - 2, sub).wait_send()

            return 0

        lax.fori_loop(0, 2, one, 0)

    def ag_came(lane, which):
        came = buf.at[which, pl.ds(theirs, half_rows)]
        pltpu.make_async_copy(came, came, ag_drecv.at[which]).wait()
        here = buf.at[which, pl.ds(mine + row_of(chip, 0, 0), share)]
        pltpu.make_async_copy(bsh.at[lane], here, ag_loc.at[lane]).wait()

    def ag_sent(lane, which):
        sent = buf.at[which, pl.ds(0, (chips - 1) * share)]
        pltpu.make_async_copy(sent, sent, ag_send.at[lane]).wait()
        over = buf.at[which, pl.ds(mine, half_rows)]
        pltpu.make_async_copy(over, over, ag_dsend.at[lane]).wait()

    def unit(lane, k):
        half, phase = lax.div(k, units // 2), lax.rem(k, 2)
        chunk = lane + 2 * lax.rem(lax.div(k, 2), chunks // 2)
        m = chunks * half + chunk
        return half, phase, chunk, m, lax.rem(m, 3)

    def lane_step(q):
        lane = lax.rem(q, 2)
        u = lax.div(q, 2) - LAG * lane

        @pl.when(u == 0)
        def _():
            rs_start(lane, unit(lane, 0)[4])

        @pl.when((u >= 1) & (u <= units * steps))
        def _():
            k, e = lax.div(u - 1, steps), lax.rem(u - 1, steps)
            half, phase, chunk, m, slot = unit(lane, k)
            s, sub = lax.div(e, SUBS), lax.rem(e, SUBS)

            @pl.when((phase == 1) & (e == AHEAD) & (k < units - 1))
            def _():
                rs_start(lane, unit(lane, k + 1)[4])

            @pl.when((phase == 0) & (s < chips - 2))
            def _():
                rs_step(lane, slot, s, sub)

            @pl.when((phase == 0) & (s == chips - 2))
            def _():
                rs_last(lane, slot, chunk, half, sub)
                ag_start(lane, m, sub)

            @pl.when((phase == 0) & (e == steps - 1) & (m + 3 < 2 * chunks))
            def _():
                pl.semaphore_signal(credit.at[slot], inc=1, **to(partner))

            @pl.when(phase == 1)
            def _():
                ag_step(lane, m, s, sub)

            @pl.when((phase == 0) & (e == 1) & (k > 0))
            def _():
                ag_sent(lane, unit(lane, k - 1)[3])

        before = 1 - lane
        v = lax.div(q + 1, 2) - 1 - LAG * before
        k = lax.div(v - 1, steps)

        @pl.when((v >= 1) & (v <= units * steps) & (lax.rem(v, steps) == 0) & (lax.rem(k, 2) == 1))
        def _():
            ag_came(before, unit(before, k)[3])

    def slots(q):
        early = a_slots
        for start, pace in ATTN:
            early += jnp.clip(lax.div((q - start) * pace, 8), 0, a_slots)
        for start, pace in MLPS:
            early += jnp.clip(lax.div((q - start) * pace, 8), 0, m_slots)
        return jnp.where(q <= 0, 0, early)

    load_act(0)
    load_w1(0)
    ga[...] = gain_a[...].astype(jnp.float32).reshape(1, d)
    gm[...] = gain_m[...].astype(jnp.float32).reshape(1, d)
    half = HEAD // 2
    pair = lax.rem(lax.broadcasted_iota(jnp.int32, (1, HEAD), 1), half).astype(jnp.float32)
    sign = jnp.where(lax.broadcasted_iota(jnp.int32, (1, HEAD), 1) < half, -1.0, 1.0)
    speed = jnp.exp(pair * (-math.log(THETA) / half))

    def table(r, _):
        at = pl.ds(pl.multiple_of(r * 64, 64), 64)
        angle = (lax.broadcasted_iota(jnp.int32, (64, HEAD), 0) + r * 64).astype(jnp.float32) * speed
        cs[at, :] = jnp.cos(angle)
        sn[at, :] = jnp.sin(angle) * sign
        return 0

    lax.fori_loop(0, rows // 64, table, 0)
    pl.semaphore_wait(barrier, 3)

    def body(q, _):
        lax.fori_loop(slots(q), slots(q + 1), compute, 0)

        @pl.when(q == 1)
        def _():
            for n in range(chunks):
                pltpu.make_async_copy(x_ref.at[n, pl.ds(mine + row_of(chip, 0, 0), share)], res.at[n], res_sem).start()

        @pl.when(q == 4)
        def _():
            pltpu.make_async_copy(res, res, res_sem).wait()

        lane_step(q)
        return 0

    lax.fori_loop(0, 2 * (units * steps + LAG + 1) + 1, body, 0)
    for lane in range(2):
        ag_sent(lane, unit(lane, units - 1)[3])
    for par in range(STAGES):
        pltpu.make_async_remote_copy(stage.at[par], land.at[0, 0], st_send.at[par], d2d_recv.at[0], **to(partner)).wait_send()


def _take(buf, y, hold, came, left):
    chunks, rows, _ = y.shape
    deep, block, _ = hold.shape
    each = rows // block
    total = chunks * each

    def copies(n):
        c, at, z = n // each, pl.ds(n % each * block, block), n % deep
        return (pltpu.make_async_copy(buf.at[chunks + c, at], hold.at[z], came.at[z]),
                pltpu.make_async_copy(hold.at[z], y.at[c, at], left.at[z]))

    for n in range(min(deep, total)):
        copies(n)[0].start()
    for n in range(total):
        copies(n)[0].wait()
        copies(n)[1].start()
        if n >= BEHIND and n - BEHIND + deep < total:
            copies(n - BEHIND)[1].wait()
            copies(n - BEHIND + deep)[0].start()
    for n in range(max(total - deep, 0), total):
        copies(n)[1].wait()


def solution(mesh):
    tp = mesh.shape["tp"]

    def step(x, gain_a, wq, wk, wv, wo, gain_m, w_gate, w_up, w_down):
        chunks, rows, d = x.shape
        chips = tp // CORES
        half_rows = rows // CORES
        share = half_rows // chips
        piece = share // (2 * SUBS)
        bf, f32 = jnp.bfloat16, jnp.float32
        vmem, dma = pltpu.VMEM, pltpu.SemaphoreType.DMA
        hbm, inside = pl.BlockSpec(memory_space=pl.ANY), pl.BlockSpec(memory_space=pltpu.VMEM)
        heads, ff = wq.shape[1] // HEAD, w_gate.shape[1]
        n_arr, n_sbuf = 2 * 2 * (chips - 1) * SUBS, 2 * 2 * 2 * SUBS
        buf = pl.pallas_call(
            functools.partial(_kernel, tp=tp),
            out_shape=jax.ShapeDtypeStruct((2 * chunks, rows, d), bf),
            in_specs=[hbm, inside, inside] + [hbm] * 7,
            out_specs=hbm,
            scratch_shapes=[
                vmem((rows, d), bf),
                vmem((3, d // WIDE, half_rows, WIDE), f32),
                vmem((3, d // WIDE, half_rows, WIDE), bf),
                vmem((STAGES, half_rows, WIDE), bf),
                vmem((n_arr, piece, d), bf),
                vmem((n_sbuf, piece, d), bf),
                vmem((chunks, share, d), bf),
                vmem((2, share, d), bf),
                vmem((DEEP, d, 256), bf),
                vmem((DEEP, ff, WIDE), bf),
                vmem((heads, rows, HEAD), bf),
                vmem((rows, HEAD), bf),
                vmem((rows, HEAD), bf),
                vmem((rows, heads * HEAD), bf),
                vmem((rows, ff), bf),
                vmem((rows, 256), f32),
                vmem((1, d), f32),
                vmem((1, d), f32),
                vmem((rows, HEAD), f32),
                vmem((rows, HEAD), f32),
                dma((PARTS,)), dma, dma((DEEP,)), dma((DEEP,)), dma((STAGES,)), dma((3,)), dma((n_sbuf,)), dma((n_arr,)), dma((2,)), dma((n_arr,)),
                dma((2,)), dma((2 * chunks,)), dma((2,)), pltpu.SemaphoreType.REGULAR((3,)),
            ],
            compiler_params=pltpu.CompilerParams(collective_id=0, has_side_effects=True, vmem_limit_bytes=66 * 10**6),
            name="layer",
        )(x, gain_a, gain_m, wq, wk, wv, wo, w_gate, w_up, w_down)
        return pl.pallas_call(
            _take,
            out_shape=jax.ShapeDtypeStruct(x.shape, bf),
            in_specs=[hbm],
            out_specs=hbm,
            scratch_shapes=[vmem((HOLD, TAKE_ROWS, d), bf), dma((HOLD,)), dma((HOLD,))],
            compiler_params=pltpu.CompilerParams(vmem_limit_bytes=66 * 10**6),
            name="take",
        )(buf)

    tokens, whole, columns, rows_of = P("dp", None, None), P(None), P(None, "tp"), P("tp", None)
    return jax.shard_map(
        step,
        mesh=mesh,
        in_specs=(tokens, whole, columns, columns, columns, rows_of, whole, columns, columns, rows_of),
        out_specs=tokens,
        check_vma=False,
    )
```
